8 devices in a mesh: dp: 1 (over z), sp: 8 (over y, x, core).
Axes of the slice: x: 2, y: 2, z: 1, core: 2. Of those that a mesh axis runs over, the one named last changes fastest.
Arguments:
- hidden: bfloat16 [16, 512, 4096], P('dp', 'sp')
- positions: int32 [512], P(('dp', 'sp'))
- long_factor: float32 [64], replicated
- norm_weight: float32 [4096], replicated
- w_qkv: bfloat16 [4096, 6144], replicated
- w_out: bfloat16 [4096, 4096], replicated
- grad_out: bfloat16 [16, 512, 4096], P('dp', 'sp')
Outputs:
- output 1: bfloat16 [16, 512, 4096], P('dp', 'sp')
- output 2: bfloat16 [16, 512, 4096], P('dp', 'sp')
- output 3: float32 [4096], P('dp')
- output 4: float32 [4096, 6144], P('dp')
- output 5: float32 [4096, 4096], P('dp')
All inputs are finite; a program needn't handle non-finite values.
Results may differ from the reference program's by a relative error of at most 0.0115151.
Values are sent between devices in bfloat16 or wider.
A program may use at most 1.25 GiB of HBM per device.

```python
import math
import jax
import jax.numpy as jnp
from jax import lax

BATCH_SIZE = 16
SEQ_LEN = 512
MODEL_DIM = 4096
NUM_HEADS = 32
KV_HEADS = 8
HEAD_DIM = 128

QUERY_DIM = NUM_HEADS * HEAD_DIM
KV_DIM = KV_HEADS * HEAD_DIM
GROUP_SIZE = NUM_HEADS // KV_HEADS
NORM_EPS = 1e-5
ROPE_BASE = 10000.0
ROPE_SCALE = math.sqrt(1.0 + math.log(32.0) / math.log(4096.0))


def setup_inputs(seed: int = 0, part: int = 0) -> dict:
    base_key = jax.random.key(seed)
    part_key = jax.random.fold_in(base_key, part)
    key_hidden, key_grad, key_pos = jax.random.split(part_key, 3)
    shared_key = jax.random.key(seed + 1)
    key_factor, key_norm, key_qkv, key_out = jax.random.split(shared_key, 4)
    hidden = jax.random.normal(key_hidden, (BATCH_SIZE, SEQ_LEN, MODEL_DIM), jnp.float32)
    grad_out = jax.random.normal(key_grad, (BATCH_SIZE, SEQ_LEN, MODEL_DIM), jnp.float32)
    pos_steps = jax.random.randint(key_pos, (SEQ_LEN,), 1, 4)
    positions = (jnp.cumsum(pos_steps) - pos_steps[0]).astype(jnp.int32)
    long_factor = jnp.exp(jax.random.uniform(key_factor, (HEAD_DIM // 2,), jnp.float32, 0.0, math.log(32.0)))
    norm_weight = 1.0 + 0.25 * jax.random.normal(key_norm, (MODEL_DIM,), jnp.float32)
    w_qkv = jax.random.normal(key_qkv, (MODEL_DIM, QUERY_DIM + 2 * KV_DIM), jnp.float32) * MODEL_DIM ** -0.5
    w_out = jax.random.normal(key_out, (QUERY_DIM, MODEL_DIM), jnp.float32) * QUERY_DIM ** -0.5
    return {'hidden': hidden.astype(jnp.bfloat16), 'positions': positions, 'long_factor': long_factor, 'norm_weight': norm_weight, 'w_qkv': w_qkv.astype(jnp.bfloat16), 'w_out': w_out.astype(jnp.bfloat16), 'grad_out': grad_out.astype(jnp.bfloat16)}


def rotate_half(head_vals):
    half_dim = HEAD_DIM // 2
    return jnp.concatenate([-head_vals[..., half_dim:], head_vals[..., :half_dim]], axis=-1)


def rope_tables(positions, long_factor):
    exponents = jnp.arange(0, HEAD_DIM, 2).astype(jnp.float32) / HEAD_DIM
    inv_freq = 1.0 / (long_factor * ROPE_BASE ** exponents)
    angles = positions.astype(jnp.float32)[:, None] * inv_freq[None, :]
    cos_half = jnp.cos(angles) * ROPE_SCALE
    sin_half = jnp.sin(angles) * ROPE_SCALE
    return jnp.concatenate([cos_half, cos_half], axis=-1), jnp.concatenate([sin_half, sin_half], axis=-1)


def apply_rope(head_vals, cos_full, sin_full):
    vals_wide = head_vals.astype(jnp.float32)
    return (vals_wide * cos_full + rotate_half(vals_wide) * sin_full).astype(jnp.bfloat16)


def attend_group(operands):
    query_grp, key_grp, value_grp = operands
    scores = jnp.einsum('bqgd,bkd->bgqk', query_grp.astype(jnp.float32), key_grp.astype(jnp.float32)) * HEAD_DIM ** -0.5
    causal = jnp.arange(SEQ_LEN)[:, None] >= jnp.arange(SEQ_LEN)[None, :]
    attn_probs = jax.nn.softmax(jnp.where(causal, scores, -jnp.inf), axis=-1).astype(jnp.bfloat16)
    return jnp.einsum('bgqk,bkd->bqgd', attn_probs.astype(jnp.float32), value_grp.astype(jnp.float32)).astype(jnp.bfloat16)


def block_forward(hidden_wide, norm_weight, w_qkv, w_out, cos_full, sin_full):
    inv_rms = lax.rsqrt(jnp.mean(hidden_wide * hidden_wide, axis=-1, keepdims=True) + NORM_EPS)
    normed = (hidden_wide * inv_rms * norm_weight).astype(jnp.bfloat16)
    qkv_proj = jnp.einsum('bsd,de->bse', normed.astype(jnp.float32), w_qkv).astype(jnp.bfloat16)
    query_raw = qkv_proj[..., :QUERY_DIM].reshape(BATCH_SIZE, SEQ_LEN, KV_HEADS, GROUP_SIZE, HEAD_DIM)
    key_raw = qkv_proj[..., QUERY_DIM:QUERY_DIM + KV_DIM].reshape(BATCH_SIZE, SEQ_LEN, KV_HEADS, HEAD_DIM)
    value_heads = qkv_proj[..., QUERY_DIM + KV_DIM:].reshape(BATCH_SIZE, SEQ_LEN, KV_HEADS, HEAD_DIM)
    query_rot = apply_rope(query_raw, cos_full[:, None, None, :], sin_full[:, None, None, :])
    key_rot = apply_rope(key_raw, cos_full[:, None, :], sin_full[:, None, :])
    attn_out = lax.map(jax.checkpoint(attend_group), (jnp.moveaxis(query_rot, 2, 0), jnp.moveaxis(key_rot, 2, 0), jnp.moveaxis(value_heads, 2, 0)))
    attn_flat = jnp.moveaxis(attn_out, 0, 2).reshape(BATCH_SIZE, SEQ_LEN, QUERY_DIM)
    mixed_out = jnp.einsum('bse,ed->bsd', attn_flat.astype(jnp.float32), w_out)
    return (hidden_wide + mixed_out).astype(jnp.bfloat16)


def reference(hidden, positions, long_factor, norm_weight, w_qkv, w_out, grad_out):
    cos_full, sin_full = rope_tables(positions, long_factor)

    def forward(hidden_wide, norm_gain, qkv_weight, out_weight):
        return block_forward(hidden_wide, norm_gain, qkv_weight, out_weight, cos_full, sin_full)

    out_hidden, pullback = jax.vjp(forward, hidden.astype(jnp.float32), norm_weight, w_qkv.astype(jnp.float32), w_out.astype(jnp.float32))
    grad_wide, grad_norm, grad_wqkv, grad_wout = pullback(grad_out)
    return out_hidden, grad_wide.astype(jnp.bfloat16), grad_norm, grad_wqkv, grad_wout
```

```python
import functools
import math
import jax
import jax.numpy as jnp
from jax import lax
from jax.experimental import pallas as pl
from jax.experimental.pallas import tpu as pltpu
from jax.sharding import PartitionSpec as P

NORM_EPS = 1e-5
ROPE_BASE = 10000.0
ROPE_SCALE = math.sqrt(1.0 + math.log(32.0) / math.log(4096.0))
LOG2_E = math.log2(math.e)
CHUNKS = (2, 4, 4, 6)


def rope_tables(positions, long_factor):
    head_dim = 2 * long_factor.shape[0]
    exponents = jnp.arange(0, head_dim, 2).astype(jnp.float32) / head_dim
    inv_freq = 1.0 / (long_factor * ROPE_BASE ** exponents)
    angles = positions.astype(jnp.float32)[:, None] * inv_freq[None, :]
    cos_half = jnp.cos(angles) * ROPE_SCALE
    sin_half = jnp.sin(angles) * ROPE_SCALE
    return jnp.concatenate([cos_half, cos_half], axis=-1), jnp.concatenate([-sin_half, sin_half], axis=-1)


def attention_kernel(qkv_ref, grad_ref, cos_ref, sin_ref, out_ref, dqkv_ref, query_s, dkey_s, dvalue_s):
    devs, _, sub, width = qkv_ref.shape
    dim = cos_ref.shape[1]
    seq = devs * sub
    group = width // dim - 2
    block = 128
    per = block // sub
    scale = dim ** -0.5
    cols = group * block

    def rope(vals, cos, sin):
        wide = vals.astype(jnp.float32)
        return (wide * cos + pltpu.roll(wide, dim // 2, 1) * sin).astype(jnp.bfloat16)

    def rope_back(vals, cos, sin):
        wide = vals.astype(jnp.float32)
        return (wide * cos - pltpu.roll(wide, dim // 2, 1) * sin).astype(jnp.bfloat16)

    def nt(lhs, rhs):
        return lax.dot_general(lhs, rhs, (((1,), (1,)), ((), ())), preferred_element_type=jnp.float32)

    def nn(lhs, rhs):
        return jnp.dot(lhs, rhs, preferred_element_type=jnp.float32)

    key_raw = qkv_ref[:, 0, :, group * dim:(group + 1) * dim].reshape(seq, dim)
    value = qkv_ref[:, 0, :, (group + 1) * dim:].reshape(seq, dim)
    key = rope(key_raw, cos_ref[...], sin_ref[...])
    key_t = key.T
    value_t = value.T
    row_ids = lax.broadcasted_iota(jnp.int32, (block, cols), 0)
    col_ids = lax.broadcasted_iota(jnp.int32, (block, cols), 1)
    allowed = row_ids <= lax.rem(col_ids, block)

    for step in reversed(range(seq // block)):
        rows = pl.ds(step * block, block)
        cos = cos_ref[rows, :]
        sin = sin_ref[rows, :]
        span = (step + 1) * block
        grads = []
        for head in range(group):
            lanes = pl.ds(head * dim, dim)
            raw = qkv_ref[step * per:(step + 1) * per, 0, :, lanes].reshape(block, dim)
            query_s[head * block:(head + 1) * block, :] = rope(raw, cos, sin)
            grads.append(grad_ref[step * per:(step + 1) * per, 0, :, lanes].reshape(block, dim))
        query = query_s[...]
        grad = jnp.concatenate(grads, axis=0)
        scores = nt(key[:span], query)
        last = jnp.where(allowed, scores[span - block:], -jnp.inf)
        scores = last if step == 0 else jnp.concatenate([scores[:span - block], last], axis=0)
        peak = jnp.max(scores, axis=0, keepdims=True)
        weights = jnp.exp2((scores - peak) * (scale * LOG2_E))
        probs = weights * (1.0 / jnp.sum(weights, axis=0, keepdims=True))
        probs_low = probs.astype(jnp.bfloat16)
        attn = nn(value_t[:, :span], probs_low).astype(jnp.bfloat16).T
        grad_probs = nt(value[:span], grad).astype(jnp.bfloat16).astype(jnp.float32)
        row_dot = jnp.sum(grad_probs * probs, axis=0, keepdims=True)
        grad_scores = (probs * (grad_probs - row_dot)).astype(jnp.bfloat16)
        grad_query = (nn(key_t[:, :span], grad_scores) * scale).astype(jnp.bfloat16).T
        part_value = nn(probs_low, grad)
        part_key = nn(grad_scores, query)
        if span == seq:
            dvalue_s[...] = part_value
            dkey_s[...] = part_key
        else:
            dvalue_s[:span, :] += part_value
            dkey_s[:span, :] += part_key
        for head in range(group):
            lanes = pl.ds(head * dim, dim)
            part = slice(head * block, (head + 1) * block)
            out_ref[step * per:(step + 1) * per, 0, :, lanes] = attn[part].reshape(per, sub, dim)
            back = rope_back(grad_query[part], cos, sin)
            dqkv_ref[step * per:(step + 1) * per, 0, :, lanes] = back.reshape(per, sub, dim)

    grad_key = (dkey_s[...] * scale).astype(jnp.bfloat16)
    back = rope_back(grad_key, cos_ref[...], sin_ref[...])
    dqkv_ref[:, 0, :, group * dim:(group + 1) * dim] = back.reshape(devs, sub, dim)
    dqkv_ref[:, 0, :, (group + 1) * dim:] = dvalue_s[...].astype(jnp.bfloat16).reshape(devs, sub, dim)


def attention(qkv, grad, cos, sin, heads, name):
    devs, count, sub, width = qkv.shape
    dim = cos.shape[1]
    seq = devs * sub
    per_head = width // heads
    group = per_head // dim - 2

    def head_spec(cols):
        return pl.BlockSpec((devs, 1, sub, cols), lambda b, a: (0, b, 0, a))

    table_spec = pl.BlockSpec((seq, dim), lambda b, a: (0, 0))
    return pl.pallas_call(
        attention_kernel,
        name=name,
        grid=(count, heads),
        in_specs=[head_spec(per_head), head_spec(group * dim), table_spec, table_spec],
        out_specs=[head_spec(group * dim), head_spec(per_head)],
        out_shape=[jax.ShapeDtypeStruct(grad.shape, jnp.bfloat16), jax.ShapeDtypeStruct(qkv.shape, jnp.bfloat16)],
        scratch_shapes=[pltpu.VMEM((group * 128, dim), jnp.bfloat16),
                        pltpu.VMEM((seq, dim), jnp.float32), pltpu.VMEM((seq, dim), jnp.float32)],
        compiler_params=pltpu.CompilerParams(vmem_limit_bytes=56 * 1024 * 1024),
        cost_estimate=pl.CostEstimate(flops=count * heads * group * 6 * 2 * seq * seq * dim,
                                      bytes_accessed=4 * (qkv.size + grad.size),
                                      transcendentals=count * heads * group * seq * seq // 2),
    )(qkv, grad, cos, sin)


def join_kernel(parts, heads, core_ref, mine_ref, other_ref, out_ref):
    first = core_ref[0] == 0
    width = sum(parts)
    start = 0
    base = 0
    for cols in parts:
        for head in range(heads):
            lanes = slice(head * width + start, head * width + start + cols)
            mine = mine_ref[:, lanes]
            other = other_ref[:, lanes]
            at = base + 2 * head * cols
            out_ref[:, at:at + cols] = jnp.where(first, mine, other)
            out_ref[:, at + cols:at + 2 * cols] = jnp.where(first, other, mine)
        start += cols
        base += 2 * heads * cols


def join_columns(core, mine, other, parts, heads, name):
    rows, half = mine.shape
    tile = 128
    spec = pl.BlockSpec((tile, half), lambda t, core_ref: (t, 0))
    return pl.pallas_call(
        functools.partial(join_kernel, parts, heads),
        name=name,
        grid_spec=pltpu.PrefetchScalarGridSpec(
            num_scalar_prefetch=1, grid=(rows // tile,), in_specs=[spec, spec],
            out_specs=pl.BlockSpec((tile, 2 * half), lambda t, core_ref: (t, 0))),
        out_shape=jax.ShapeDtypeStruct((rows, 2 * half), mine.dtype),
        compiler_params=pltpu.CompilerParams(vmem_limit_bytes=40 * 1024 * 1024),
        cost_estimate=pl.CostEstimate(flops=rows * half * 64, bytes_accessed=4 * rows * half * mine.dtype.itemsize,
                                      transcendentals=0),
    )(core, mine, other)


def pick_columns_kernel(core_ref, query_ref, key_ref, value_ref, out_ref):
    query = query_ref.shape[1]
    small = key_ref.shape[1]
    out_ref[:, :query] = query_ref[...]
    out_ref[:, query:query + small] = key_ref[...]
    out_ref[:, query + small:] = value_ref[...]


def pick_columns(core, w_qkv, heads, group, dim):
    rows = w_qkv.shape[0]
    tile = 1024
    width = (group + 2) * dim
    kv_base = 2 * heads * group
    return pl.pallas_call(
        pick_columns_kernel,
        name='pick_columns',
        grid_spec=pltpu.PrefetchScalarGridSpec(
            num_scalar_prefetch=1, grid=(rows // tile, heads),
            in_specs=[pl.BlockSpec((tile, group * dim), lambda t, a, core_ref: (t, 2 * a + core_ref[0])),
                      pl.BlockSpec((tile, dim), lambda t, a, core_ref: (t, kv_base + 2 * a + core_ref[0])),
                      pl.BlockSpec((tile, dim), lambda t, a, core_ref: (t, kv_base + 2 * heads + 2 * a + core_ref[0]))],
            out_specs=pl.BlockSpec((tile, width), lambda t, a, core_ref: (t, a))),
        out_shape=jax.ShapeDtypeStruct((rows, heads * width), w_qkv.dtype),
        compiler_params=pltpu.CompilerParams(vmem_limit_bytes=32 * 1024 * 1024),
        cost_estimate=pl.CostEstimate(flops=rows * heads * width * 32, bytes_accessed=4 * rows * heads * width,
                                      transcendentals=0),
    )(core, w_qkv, w_qkv, w_qkv)


def pick_rows_kernel(core_ref, in_ref, out_ref):
    out_ref[...] = in_ref[...]


def pick_rows(core, w_out, heads, rows):
    cols = w_out.shape[1]
    return pl.pallas_call(
        pick_rows_kernel,
        name='pick_rows',
        grid_spec=pltpu.PrefetchScalarGridSpec(
            num_scalar_prefetch=1, grid=(heads, 2),
            in_specs=[pl.BlockSpec((rows // 2, cols), lambda a, h, core_ref: (4 * a + 2 * core_ref[0] + h, 0))],
            out_specs=pl.BlockSpec((rows // 2, cols), lambda a, h, core_ref: (2 * a + h, 0))),
        out_shape=jax.ShapeDtypeStruct((heads * rows, cols), w_out.dtype),
        compiler_params=pltpu.CompilerParams(vmem_limit_bytes=32 * 1024 * 1024),
        cost_estimate=pl.CostEstimate(flops=heads * rows * cols * 32, bytes_accessed=4 * heads * rows * cols,
                                      transcendentals=0),
    )(core, w_out)


def pick_tokens_kernel(count, devs_ref, *refs):
    inputs, outputs = refs[:2 * count], refs[2 * count:]
    for side in range(2):
        start = 0
        for index in range(count):
            part = inputs[side * count + index]
            outputs[side][start:start + part.shape[1]] = part[0]
            start += part.shape[1]


def pick_tokens(devs, chunks, name):
    sub, width = chunks[0].shape[2:]
    batch = sum(chunk.shape[1] for chunk in chunks)

    def token_spec(chunk, side):
        return pl.BlockSpec((1,) + chunk.shape[1:], lambda g, devs_ref: (devs_ref[side], 0, 0, 0))

    out = jax.ShapeDtypeStruct((batch, sub, width), chunks[0].dtype)
    out_spec = pl.BlockSpec((batch, sub, width), lambda g, devs_ref: (0, 0, 0))
    return pl.pallas_call(
        functools.partial(pick_tokens_kernel, len(chunks)),
        name=name,
        grid_spec=pltpu.PrefetchScalarGridSpec(
            num_scalar_prefetch=1, grid=(1,),
            in_specs=[token_spec(chunk, side) for side in range(2) for chunk in chunks],
            out_specs=[out_spec, out_spec]),
        out_shape=[out, out],
        compiler_params=pltpu.CompilerParams(vmem_limit_bytes=60 * 1024 * 1024),
        cost_estimate=pl.CostEstimate(flops=batch * sub * width * 64, bytes_accessed=8 * batch * sub * width,
                                      transcendentals=0),
    )(devs, *chunks, *chunks)


def block_body(hidden, positions, long_factor, norm_weight, w_qkv, w_out, grad_out):
    batch, sub, model = hidden.shape
    dim = 2 * long_factor.shape[0]
    query_dim = w_out.shape[0]
    kv_dim = (w_qkv.shape[1] - query_dim) // 2
    kv_heads = kv_dim // dim
    group = query_dim // kv_dim
    devs = lax.axis_size('sp')
    mine_heads = kv_heads // 2
    me = lax.axis_index('sp')
    core = lax.rem(me, 2)
    chip = lax.div(me, 2)
    partner = me + 1 - 2 * core
    pairs = [(d, d ^ 1) for d in range(devs)]

    hidden_wide = hidden.astype(jnp.float32)
    inv_rms = lax.rsqrt(jnp.mean(hidden_wide * hidden_wide, axis=-1, keepdims=True) + NORM_EPS)
    normed = (hidden_wide * inv_rms * norm_weight).astype(jnp.bfloat16)

    core_ref = core.reshape(1)
    w_own = pick_columns(core_ref, w_qkv, mine_heads, group, dim)
    wo_own = pick_rows(core_ref, w_out, mine_heads, group * dim)
    cos, sin = rope_tables(lax.all_gather(positions, 'sp', axis=0, tiled=True), long_factor)

    gathered = []
    start = 0
    for count in CHUNKS:
        gathered.append((lax.all_gather(normed[start:start + count], 'sp', axis=0),
                         lax.all_gather(grad_out[start:start + count], 'sp', axis=0)))
        start += count

    grad_wqkv = None
    grad_wout = None
    tokens = []
    for index, (normed_all, grad_all) in enumerate(gathered):
        qkv = jnp.einsum('tbsd,de->tbse', normed_all, w_own, preferred_element_type=jnp.float32).astype(jnp.bfloat16)
        grad_attn = jnp.einsum('tbsd,ed->tbse', grad_all, wo_own, preferred_element_type=jnp.float32).astype(jnp.bfloat16)
        attn, grad_qkv = attention(qkv, grad_attn, cos, sin, mine_heads, f'attention_{index}')
        attn_slice = lax.dynamic_slice_in_dim(attn, chip * group * dim, group * dim, axis=3)
        part_out = jnp.einsum('tbse,tbsd->ed', attn_slice, grad_all, preferred_element_type=jnp.float32)
        part_qkv = jnp.einsum('tbsd,tbse->de', normed_all, grad_qkv, preferred_element_type=jnp.float32)
        grad_wout = part_out if grad_wout is None else grad_wout + part_out
        grad_wqkv = part_qkv if grad_wqkv is None else grad_wqkv + part_qkv
        tokens.append((attn, grad_qkv))

    grad_wout = lax.all_gather(grad_wout, 'sp', axis=0, tiled=True)
    grad_wqkv_other = lax.ppermute(grad_wqkv, 'sp', pairs)

    ends = jnp.stack([me, partner])
    attn_mine, attn_send = pick_tokens(ends, [pair[0] for pair in tokens], 'pick_attention')
    dqkv_mine, dqkv_send = pick_tokens(ends, [pair[1] for pair in tokens], 'pick_gradient')
    attn_other = lax.ppermute(attn_send, 'sp', pairs)
    dqkv_other = lax.ppermute(dqkv_send, 'sp', pairs)

    def natural(mine, other, parts, name):
        rows = (batch * sub, -1)
        joined = join_columns(core_ref, mine.reshape(rows), other.reshape(rows), parts, mine_heads, name)
        return joined.reshape(batch, sub, -1)

    parts = (group * dim, dim, dim)
    attn_flat = natural(attn_mine, attn_other, parts[:1], 'join_attention')
    mixed_out = jnp.einsum('bse,ed->bsd', attn_flat, w_out, preferred_element_type=jnp.float32)
    out_hidden = (hidden_wide + mixed_out).astype(jnp.bfloat16)

    grad_qkv = natural(dqkv_mine, dqkv_other, parts, 'join_gradient')
    grad_normed = jnp.einsum('bse,de->bsd', grad_qkv, w_qkv, preferred_element_type=jnp.float32)
    grad_normed = grad_normed.astype(jnp.bfloat16).astype(jnp.float32)
    unit_hidden = hidden_wide * inv_rms
    grad_norm = jnp.sum(grad_normed * unit_hidden, axis=(0, 1))
    grad_unit = grad_normed * norm_weight
    grad_inner = inv_rms * (grad_unit - unit_hidden * jnp.mean(grad_unit * unit_hidden, axis=-1, keepdims=True))
    grad_hidden = (grad_out.astype(jnp.float32) + grad_inner).astype(jnp.bfloat16)

    grad_wqkv = join_columns(core_ref, grad_wqkv, grad_wqkv_other, parts, mine_heads, 'join_weights')
    return out_hidden, grad_hidden, lax.psum(grad_norm, 'sp'), grad_wqkv, grad_wout


def solution(mesh):
    token_spec = P('dp', 'sp', None)
    return jax.shard_map(block_body, mesh=mesh,
                         in_specs=(token_spec, P(('dp', 'sp')), P(), P(), P(), P(), token_spec),
                         out_specs=(token_spec, token_spec, P('dp'), P('dp', None), P('dp', None)),
                         check_vma=False)
```

```python
import functools
import math
import jax
import jax.numpy as jnp
from jax import lax
from jax.experimental import pallas as pl
from jax.experimental.pallas import tpu as pltpu
from jax.sharding import PartitionSpec as P

NORM_EPS = 1e-5
ROPE_BASE = 10000.0
ROPE_SCALE = math.sqrt(1.0 + math.log(32.0) / math.log(4096.0))
LOG2_E = math.log2(math.e)
CHUNKS = (2, 5, 5, 4)


def rope_tables(positions, long_factor):
    head_dim = 2 * long_factor.shape[0]
    exponents = jnp.arange(0, head_dim, 2).astype(jnp.float32) / head_dim
    inv_freq = 1.0 / (long_factor * ROPE_BASE ** exponents)
    angles = positions.astype(jnp.float32)[:, None] * inv_freq[None, :]
    cos_half = jnp.cos(angles) * ROPE_SCALE
    sin_half = jnp.sin(angles) * ROPE_SCALE
    return jnp.concatenate([cos_half, cos_half], axis=-1), jnp.concatenate([-sin_half, sin_half], axis=-1)


def attention_kernel(qkv_ref, grad_ref, cos_ref, sin_ref, out_ref, dquery_ref, dkv_ref, dkey_s, dvalue_s):
    devs, _, sub, width = qkv_ref.shape
    dim = cos_ref.shape[1]
    seq = devs * sub
    group = width // dim - 2
    block = 128
    per = block // sub
    scale = dim ** -0.5

    def rope(vals, cos, sin):
        wide = vals.astype(jnp.float32)
        return (wide * cos + pltpu.roll(wide, dim // 2, 1) * sin).astype(jnp.bfloat16)

    def rope_back(vals, cos, sin):
        wide = vals.astype(jnp.float32)
        return (wide * cos - pltpu.roll(wide, dim // 2, 1) * sin).astype(jnp.bfloat16)

    def nt(lhs, rhs):
        return lax.dot_general(lhs, rhs, (((1,), (1,)), ((), ())), preferred_element_type=jnp.float32)

    def nn(lhs, rhs):
        return jnp.dot(lhs, rhs, preferred_element_type=jnp.float32)

    key_raw = qkv_ref[:, 0, :, group * dim:(group + 1) * dim].reshape(seq, dim)
    value = qkv_ref[:, 0, :, (group + 1) * dim:].reshape(seq, dim)
    key = rope(key_raw, cos_ref[...], sin_ref[...])
    key_t = key.T
    value_t = value.T
    heads_unit = 2
    cols = heads_unit * block
    row_ids = lax.broadcasted_iota(jnp.int32, (block, cols), 0)
    col_ids = lax.broadcasted_iota(jnp.int32, (block, cols), 1)
    allowed = row_ids <= lax.rem(col_ids, block)
    units = [(step, first) for step in reversed(range(seq // block)) for first in range(0, group, heads_unit)]
    state = {}

    def load(unit):
        step, first = units[unit]
        rows = pl.ds(step * block, block)
        cos = cos_ref[rows, :]
        sin = sin_ref[rows, :]
        span = (step + 1) * block
        queries = []
        grads = []
        for head in range(first, first + heads_unit):
            lanes = pl.ds(head * dim, dim)
            raw = qkv_ref[step * per:(step + 1) * per, 0, :, lanes].reshape(block, dim)
            queries.append(rope(raw, cos, sin))
            grads.append(grad_ref[step * per:(step + 1) * per, 0, :, lanes].reshape(block, dim))
        query = jnp.concatenate(queries, axis=0)
        grad = jnp.concatenate(grads, axis=0)
        scores = nt(key[:span], query)
        grad_probs = nt(value[:span], grad).astype(jnp.bfloat16)
        state[unit] = (query, grad, scores, grad_probs)

    def soften(unit):
        step, first = units[unit]
        span = (step + 1) * block
        query, grad, scores, grad_probs = state[unit]
        last = jnp.where(allowed, scores[span - block:], -jnp.inf)
        scores = last if step == 0 else jnp.concatenate([scores[:span - block], last], axis=0)
        peak = jnp.max(scores, axis=0, keepdims=True)
        weights = jnp.exp2((scores - peak) * (scale * LOG2_E))
        probs = weights * (1.0 / jnp.sum(weights, axis=0, keepdims=True))
        grad_probs = grad_probs.astype(jnp.float32)
        row_dot = jnp.sum(grad_probs * probs, axis=0, keepdims=True)
        grad_scores = (probs * (grad_probs - row_dot)).astype(jnp.bfloat16)
        state[unit] = (query, grad, probs.astype(jnp.bfloat16), grad_scores)

    def finish(unit):
        step, first = units[unit]
        rows = pl.ds(step * block, block)
        cos = cos_ref[rows, :]
        sin = sin_ref[rows, :]
        span = (step + 1) * block
        query, grad, probs_low, grad_scores = state.pop(unit)
        attn = nn(value_t[:, :span], probs_low).astype(jnp.bfloat16).T
        grad_query = (nn(key_t[:, :span], grad_scores) * scale).astype(jnp.bfloat16).T
        part_value = nn(probs_low, grad)
        part_key = nn(grad_scores, query)
        if unit == 0:
            dvalue_s[...] = part_value
            dkey_s[...] = part_key
        else:
            dvalue_s[:span, :] += part_value
            dkey_s[:span, :] += part_key
        for head in range(heads_unit):
            lanes = pl.ds((first + head) * dim, dim)
            part = slice(head * block, (head + 1) * block)
            out_ref[step * per:(step + 1) * per, 0, :, lanes] = attn[part].reshape(per, sub, dim)
            back = rope_back(grad_query[part], cos, sin)
            dquery_ref[step * per:(step + 1) * per, 0, :, lanes] = back.reshape(per, sub, dim)

    count = len(units)
    load(0)
    for unit in range(count + 1):
        if unit < count:
            soften(unit)
        if unit + 1 < count:
            load(unit + 1)
        if unit > 0:
            finish(unit - 1)

    grad_key = (dkey_s[...] * scale).astype(jnp.bfloat16)
    back = rope_back(grad_key, cos_ref[...], sin_ref[...])
    dkv_ref[:, 0, :, :dim] = back.reshape(devs, sub, dim)
    dkv_ref[:, 0, :, dim:] = dvalue_s[...].astype(jnp.bfloat16).reshape(devs, sub, dim)


def attention(qkv, grad, cos, sin, heads, name):
    devs, count, sub, width = qkv.shape
    dim = cos.shape[1]
    seq = devs * sub
    per_head = width // heads
    group = per_head // dim - 2

    def head_spec(cols):
        return pl.BlockSpec((devs, 1, sub, cols), lambda b, a: (0, b, 0, a))

    table_spec = pl.BlockSpec((seq, dim), lambda b, a: (0, 0))
    return pl.pallas_call(
        attention_kernel,
        name=name,
        grid=(count, heads),
        in_specs=[head_spec(per_head), head_spec(group * dim), table_spec, table_spec],
        out_specs=[head_spec(group * dim), head_spec(group * dim), head_spec(2 * dim)],
        out_shape=[jax.ShapeDtypeStruct((devs, count, sub, heads * cols), jnp.bfloat16)
                   for cols in (group * dim, group * dim, 2 * dim)],
        scratch_shapes=[pltpu.VMEM((seq, dim), jnp.float32), pltpu.VMEM((seq, dim), jnp.float32)],
        compiler_params=pltpu.CompilerParams(vmem_limit_bytes=56 * 1024 * 1024),
        cost_estimate=pl.CostEstimate(flops=count * heads * group * 6 * 2 * seq * seq * dim,
                                      bytes_accessed=4 * (qkv.size + grad.size),
                                      transcendentals=count * heads * group * seq * seq // 2),
    )(qkv, grad, cos, sin)


def join_kernel(parts, heads, core_ref, *refs):
    first = core_ref[0] == 0
    out_ref = refs[-1]
    base = 0
    for index, group_parts in enumerate(parts):
        mine_ref, other_ref = refs[2 * index], refs[2 * index + 1]
        width = sum(group_parts)
        start = 0
        for cols in group_parts:
            for head in range(heads):
                lanes = slice(head * width + start, head * width + start + cols)
                mine = mine_ref[:, lanes]
                other = other_ref[:, lanes]
                at = base + 2 * head * cols
                out_ref[:, at:at + cols] = jnp.where(first, mine, other)
                out_ref[:, at + cols:at + 2 * cols] = jnp.where(first, other, mine)
            start += cols
            base += 2 * heads * cols


def join_columns(core, pairs, parts, heads, name):
    arrays = [array for pair in pairs for array in pair]
    rows = arrays[0].shape[0]
    total = sum(array.shape[1] for array in arrays)
    tile = 128
    return pl.pallas_call(
        functools.partial(join_kernel, parts, heads),
        name=name,
        grid_spec=pltpu.PrefetchScalarGridSpec(
            num_scalar_prefetch=1, grid=(rows // tile,),
            in_specs=[pl.BlockSpec((tile, array.shape[1]), lambda t, core_ref: (t, 0)) for array in arrays],
            out_specs=pl.BlockSpec((tile, total), lambda t, core_ref: (t, 0))),
        out_shape=jax.ShapeDtypeStruct((rows, total), arrays[0].dtype),
        compiler_params=pltpu.CompilerParams(vmem_limit_bytes=40 * 1024 * 1024),
        cost_estimate=pl.CostEstimate(flops=rows * total * 32, bytes_accessed=2 * rows * total * arrays[0].dtype.itemsize,
                                      transcendentals=0),
    )(core, *arrays)


def join_weights_kernel(heads, core_ref, mine_ref, other_ref, kv_ref, out_ref):
    first = core_ref[0] == 0
    cols = mine_ref.shape[1] // heads
    dim = kv_ref.shape[2] // 2
    for head in range(heads):
        lanes = slice(head * cols, (head + 1) * cols)
        mine = mine_ref[:, lanes]
        other = other_ref[:, lanes]
        at = 2 * head * cols
        out_ref[:, at:at + cols] = jnp.where(first, mine, other)
        out_ref[:, at + cols:at + 2 * cols] = jnp.where(first, other, mine)
    base = 2 * heads * cols
    for head in range(2 * heads):
        out_ref[:, base + head * dim:base + (head + 1) * dim] = kv_ref[head, :, :dim]
        at = base + (2 * heads + head) * dim
        out_ref[:, at:at + dim] = kv_ref[head, :, dim:]


def join_weights(core, mine, other, kv_all, heads):
    rows, half = mine.shape
    total = 2 * half + kv_all.shape[0] * kv_all.shape[2]
    tile = 128
    spec = pl.BlockSpec((tile, half), lambda t, core_ref: (t, 0))
    return pl.pallas_call(
        functools.partial(join_weights_kernel, heads),
        name='join_weights',
        grid_spec=pltpu.PrefetchScalarGridSpec(
            num_scalar_prefetch=1, grid=(rows // tile,),
            in_specs=[spec, spec,
                      pl.BlockSpec((kv_all.shape[0], tile, kv_all.shape[2]), lambda t, core_ref: (0, t, 0))],
            out_specs=pl.BlockSpec((tile, total), lambda t, core_ref: (t, 0))),
        out_shape=jax.ShapeDtypeStruct((rows, total), mine.dtype),
        compiler_params=pltpu.CompilerParams(vmem_limit_bytes=40 * 1024 * 1024),
        cost_estimate=pl.CostEstimate(flops=rows * total * 32, bytes_accessed=8 * rows * total, transcendentals=0),
    )(core, mine, other, kv_all)


def pick_columns_kernel(core_ref, query_ref, key_ref, value_ref, out_ref):
    query = query_ref.shape[1]
    small = key_ref.shape[1]
    out_ref[:, :query] = query_ref[...]
    out_ref[:, query:query + small] = key_ref[...]
    out_ref[:, query + small:] = value_ref[...]


def pick_columns(core, w_qkv, heads, group, dim):
    rows = w_qkv.shape[0]
    tile = 1024
    width = (group + 2) * dim
    kv_base = 2 * heads * group
    return pl.pallas_call(
        pick_columns_kernel,
        name='pick_columns',
        grid_spec=pltpu.PrefetchScalarGridSpec(
            num_scalar_prefetch=1, grid=(rows // tile, heads),
            in_specs=[pl.BlockSpec((tile, group * dim), lambda t, a, core_ref: (t, 2 * a + core_ref[0])),
                      pl.BlockSpec((tile, dim), lambda t, a, core_ref: (t, kv_base + 2 * a + core_ref[0])),
                      pl.BlockSpec((tile, dim), lambda t, a, core_ref: (t, kv_base + 2 * heads + 2 * a + core_ref[0]))],
            out_specs=pl.BlockSpec((tile, width), lambda t, a, core_ref: (t, a))),
        out_shape=jax.ShapeDtypeStruct((rows, heads * width), w_qkv.dtype),
        compiler_params=pltpu.CompilerParams(vmem_limit_bytes=32 * 1024 * 1024),
        cost_estimate=pl.CostEstimate(flops=rows * heads * width * 32, bytes_accessed=4 * rows * heads * width,
                                      transcendentals=0),
    )(core, w_qkv, w_qkv, w_qkv)


def pick_rows_kernel(core_ref, in_ref, out_ref):
    out_ref[...] = in_ref[...]


def pick_rows(core, w_out, heads, rows):
    cols = w_out.shape[1]
    return pl.pallas_call(
        pick_rows_kernel,
        name='pick_rows',
        grid_spec=pltpu.PrefetchScalarGridSpec(
            num_scalar_prefetch=1, grid=(heads, 2),
            in_specs=[pl.BlockSpec((rows // 2, cols), lambda a, h, core_ref: (4 * a + 2 * core_ref[0] + h, 0))],
            out_specs=pl.BlockSpec((rows // 2, cols), lambda a, h, core_ref: (2 * a + h, 0))),
        out_shape=jax.ShapeDtypeStruct((heads * rows, cols), w_out.dtype),
        compiler_params=pltpu.CompilerParams(vmem_limit_bytes=32 * 1024 * 1024),
        cost_estimate=pl.CostEstimate(flops=heads * rows * cols * 32, bytes_accessed=4 * heads * rows * cols,
                                      transcendentals=0),
    )(core, w_out)


def pick_tokens_kernel(count, devs_ref, *refs):
    inputs, outputs = refs[:2 * count], refs[2 * count:]
    for side in range(2):
        start = 0
        for index in range(count):
            part = inputs[side * count + index]
            outputs[side][start:start + part.shape[1]] = part[0]
            start += part.shape[1]


def pick_tokens(devs, chunks, name):
    sub, width = chunks[0].shape[2:]
    batch = sum(chunk.shape[1] for chunk in chunks)

    def token_spec(chunk, side):
        return pl.BlockSpec((1,) + chunk.shape[1:], lambda g, devs_ref: (devs_ref[side], 0, 0, 0))

    out = jax.ShapeDtypeStruct((batch, sub, width), chunks[0].dtype)
    out_spec = pl.BlockSpec((batch, sub, width), lambda g, devs_ref: (0, 0, 0))
    return pl.pallas_call(
        functools.partial(pick_tokens_kernel, len(chunks)),
        name=name,
        grid_spec=pltpu.PrefetchScalarGridSpec(
            num_scalar_prefetch=1, grid=(1,),
            in_specs=[token_spec(chunk, side) for side in range(2) for chunk in chunks],
            out_specs=[out_spec, out_spec]),
        out_shape=[out, out],
        compiler_params=pltpu.CompilerParams(vmem_limit_bytes=60 * 1024 * 1024),
        cost_estimate=pl.CostEstimate(flops=batch * sub * width * 64, bytes_accessed=8 * batch * sub * width,
                                      transcendentals=0),
    )(devs, *chunks, *chunks)


def exchange_sum(part, devs):
    bit = 1
    while bit < devs:
        part = part + lax.ppermute(part, 'sp', [(d, d ^ bit) for d in range(devs)])
        bit *= 2
    return part


def block_body(hidden, positions, long_factor, norm_weight, w_qkv, w_out, grad_out):
    batch, sub, model = hidden.shape
    dim = 2 * long_factor.shape[0]
    query_dim = w_out.shape[0]
    kv_dim = (w_qkv.shape[1] - query_dim) // 2
    kv_heads = kv_dim // dim
    group = query_dim // kv_dim
    devs = lax.axis_size('sp')
    mine_heads = kv_heads // 2
    me = lax.axis_index('sp')
    core = lax.rem(me, 2)
    chip = lax.div(me, 2)
    partner = me + 1 - 2 * core
    pairs = [(d, d ^ 1) for d in range(devs)]

    hidden_wide = hidden.astype(jnp.float32)
    inv_rms = lax.rsqrt(jnp.mean(hidden_wide * hidden_wide, axis=-1, keepdims=True) + NORM_EPS)
    normed = (hidden_wide * inv_rms * norm_weight).astype(jnp.bfloat16)

    core_ref = core.reshape(1)
    w_own = pick_columns(core_ref, w_qkv, mine_heads, group, dim)
    wo_own = pick_rows(core_ref, w_out, mine_heads, group * dim)
    spread = lax.dynamic_update_slice(jnp.zeros((devs * sub,), positions.dtype), positions, (me * sub,))
    cos, sin = rope_tables(exchange_sum(spread, devs), long_factor)

    gathered = []
    start = 0
    for count in CHUNKS:
        gathered.append((lax.all_gather(normed[start:start + count], 'sp', axis=0),
                         lax.all_gather(grad_out[start:start + count], 'sp', axis=0)))
        start += count

    grad_wq = []
    grad_wkv = None
    grad_wout = None
    tokens = []
    last = len(CHUNKS) - 1
    for index, (normed_all, grad_all) in enumerate(gathered):
        if index > 0:
            attn, grad_all = lax.optimization_barrier((tokens[-1][0], grad_all))
            tokens[-1] = (attn,) + tokens[-1][1:]
        grad_attn = jnp.einsum('tbsd,ed->tbse', grad_all, wo_own, preferred_element_type=jnp.float32).astype(jnp.bfloat16)
        grad_attn, normed_all = lax.optimization_barrier((grad_attn, normed_all))
        if index == 1:
            grad_wq[-1], grad_wkv, grad_wout, normed_all = lax.optimization_barrier(
                (grad_wq[-1], grad_wkv, grad_wout, normed_all))
        qkv = jnp.einsum('tbsd,de->tbse', normed_all, w_own, preferred_element_type=jnp.float32).astype(jnp.bfloat16)
        attn, grad_query, grad_kv = attention(qkv, grad_attn, cos, sin, mine_heads, f'attention_{index}')
        tokens.append((attn, grad_query, grad_kv))
        kv_slice = lax.dynamic_slice_in_dim(grad_kv, chip * 2 * dim, 2 * dim, axis=3)
        part_kv = jnp.einsum('tbsd,tbse->de', normed_all, kv_slice, preferred_element_type=jnp.float32)
        grad_wkv = part_kv if grad_wkv is None else grad_wkv + part_kv
        attn_slice = lax.dynamic_slice_in_dim(attn, chip * group * dim, group * dim, axis=3)
        if index == last:
            grad_wkv, attn_slice = lax.optimization_barrier((grad_wkv, attn_slice))
        part_out = jnp.einsum('tbse,tbsd->ed', attn_slice, grad_all, preferred_element_type=jnp.float32)
        grad_wout = part_out if grad_wout is None else grad_wout + part_out
        if index == last:
            ends = jnp.stack([me, partner])
            picked = [pick_tokens(ends, list(parts), name) for parts, name in
                      zip(zip(*tokens), ('pick_attention', 'pick_query', 'pick_kv'))]
            others = [lax.ppermute(pair[1], 'sp', pairs) for pair in picked]
            *others, grad_query = lax.optimization_barrier((*others, grad_query))
        part_q = jnp.einsum('tbsd,tbse->de', normed_all, grad_query, preferred_element_type=jnp.float32)
        grad_wq.append(part_q if not grad_wq else grad_wq[-1] + part_q)

    grad_wq_other = lax.ppermute(grad_wq[-1], 'sp', pairs)
    grad_wkv_all = lax.all_gather(grad_wkv, 'sp', axis=0)
    grad_wout = lax.all_gather(grad_wout, 'sp', axis=0, tiled=True)

    def natural(indices, parts, name):
        rows = (batch * sub, -1)
        joined = join_columns(core_ref, [(picked[i][0].reshape(rows), others[i].reshape(rows)) for i in indices],
                              parts, mine_heads, name)
        return joined.reshape(batch, sub, -1)

    attn_flat = natural((0,), ((group * dim,),), 'join_attention')
    mixed_out = jnp.einsum('bse,ed->bsd', attn_flat, w_out, preferred_element_type=jnp.float32)
    out_hidden = (hidden_wide + mixed_out).astype(jnp.bfloat16)

    grad_qkv = natural((1, 2), ((group * dim,), (dim, dim)), 'join_gradient')
    grad_normed = jnp.einsum('bse,de->bsd', grad_qkv, w_qkv, preferred_element_type=jnp.float32)
    grad_normed = grad_normed.astype(jnp.bfloat16).astype(jnp.float32)
    unit_hidden = hidden_wide * inv_rms
    grad_norm = jnp.sum(grad_normed * unit_hidden, axis=(0, 1))
    grad_unit = grad_normed * norm_weight
    grad_inner = inv_rms * (grad_unit - unit_hidden * jnp.mean(grad_unit * unit_hidden, axis=-1, keepdims=True))
    grad_hidden = (grad_out.astype(jnp.float32) + grad_inner).astype(jnp.bfloat16)

    grad_wqkv = join_weights(core_ref, grad_wq[-1], grad_wq_other, grad_wkv_all, mine_heads)
    return out_hidden, grad_hidden, exchange_sum(grad_norm, devs), grad_wqkv, grad_wout


def solution(mesh):
    token_spec = P('dp', 'sp', None)
    return jax.shard_map(block_body, mesh=mesh,
                         in_specs=(token_spec, P(('dp', 'sp')), P(), P(), P(), P(), token_spec),
                         out_specs=(token_spec, token_spec, P('dp'), P('dp', None), P('dp', None)),
                         check_vma=False)
```

```python
import functools
import math
import jax
import jax.numpy as jnp
from jax import lax
from jax.experimental import pallas as pl
from jax.experimental.pallas import tpu as pltpu
from jax.sharding import PartitionSpec as P

NORM_EPS = 1e-5
ROPE_BASE = 10000.0
ROPE_SCALE = math.sqrt(1.0 + math.log(32.0) / math.log(4096.0))
LOG2_E = math.log2(math.e)
CHUNKS = (2, 4, 5, 5)


def rope_tables(positions, long_factor):
    head_dim = 2 * long_factor.shape[0]
    exponents = jnp.arange(0, head_dim, 2).astype(jnp.float32) / head_dim
    inv_freq = 1.0 / (long_factor * ROPE_BASE ** exponents)
    angles = positions.astype(jnp.float32)[:, None] * inv_freq[None, :]
    cos_half = jnp.cos(angles) * ROPE_SCALE
    sin_half = jnp.sin(angles) * ROPE_SCALE
    return jnp.concatenate([cos_half, cos_half], axis=-1), jnp.concatenate([-sin_half, sin_half], axis=-1)


def attention_kernel(qkv_ref, grad_ref, cos_ref, sin_ref, out_ref, dqkv_ref, dkey_s, dvalue_s):
    devs, _, sub, width = qkv_ref.shape
    dim = cos_ref.shape[1]
    seq = devs * sub
    group = width // dim - 2
    block = 128
    per = block // sub
    scale = dim ** -0.5

    def rope(vals, cos, sin):
        wide = vals.astype(jnp.float32)
        return (wide * cos + pltpu.roll(wide, dim // 2, 1) * sin).astype(jnp.bfloat16)

    def rope_back(vals, cos, sin):
        wide = vals.astype(jnp.float32)
        return (wide * cos - pltpu.roll(wide, dim // 2, 1) * sin).astype(jnp.bfloat16)

    def nt(lhs, rhs):
        return lax.dot_general(lhs, rhs, (((1,), (1,)), ((), ())), preferred_element_type=jnp.float32)

    def nn(lhs, rhs):
        return jnp.dot(lhs, rhs, preferred_element_type=jnp.float32)

    key_raw = qkv_ref[:, 0, :, group * dim:(group + 1) * dim].reshape(seq, dim)
    value = qkv_ref[:, 0, :, (group + 1) * dim:].reshape(seq, dim)
    key = rope(key_raw, cos_ref[...], sin_ref[...])
    key_t = key.T
    value_t = value.T
    heads_unit = 2
    cols = heads_unit * block
    row_ids = lax.broadcasted_iota(jnp.int32, (block, cols), 0)
    col_ids = lax.broadcasted_iota(jnp.int32, (block, cols), 1)
    allowed = row_ids <= lax.rem(col_ids, block)
    units = [(step, first) for step in reversed(range(seq // block)) for first in range(0, group, heads_unit)]
    state = {}

    def load(unit):
        step, first = units[unit]
        rows = pl.ds(step * block, block)
        cos = cos_ref[rows, :]
        sin = sin_ref[rows, :]
        span = (step + 1) * block
        queries = []
        grads = []
        for head in range(first, first + heads_unit):
            lanes = pl.ds(head * dim, dim)
            raw = qkv_ref[step * per:(step + 1) * per, 0, :, lanes].reshape(block, dim)
            queries.append(rope(raw, cos, sin))
            grads.append(grad_ref[step * per:(step + 1) * per, 0, :, lanes].reshape(block, dim))
        query = jnp.concatenate(queries, axis=0)
        grad = jnp.concatenate(grads, axis=0)
        scores = nt(key[:span], query)
        grad_probs = nt(value[:span], grad).astype(jnp.bfloat16)
        state[unit] = (query, grad, scores, grad_probs)

    def soften(unit):
        step, first = units[unit]
        span = (step + 1) * block
        query, grad, scores, grad_probs = state[unit]
        last = jnp.where(allowed, scores[span - block:], -jnp.inf)
        scores = last if step == 0 else jnp.concatenate([scores[:span - block], last], axis=0)
        peak = jnp.max(scores, axis=0, keepdims=True)
        weights = jnp.exp2((scores - peak) * (scale * LOG2_E))
        probs = weights * (1.0 / jnp.sum(weights, axis=0, keepdims=True))
        grad_probs = grad_probs.astype(jnp.float32)
        row_dot = jnp.sum(grad_probs * probs, axis=0, keepdims=True)
        grad_scores = (probs * (grad_probs - row_dot)).astype(jnp.bfloat16)
        state[unit] = (query, grad, probs.astype(jnp.bfloat16), grad_scores)

    def finish(unit):
        step, first = units[unit]
        rows = pl.ds(step * block, block)
        cos = cos_ref[rows, :]
        sin = sin_ref[rows, :]
        span = (step + 1) * block
        query, grad, probs_low, grad_scores = state.pop(unit)
        attn = nn(value_t[:, :span], probs_low).astype(jnp.bfloat16).T
        grad_query = (nn(key_t[:, :span], grad_scores) * scale).astype(jnp.bfloat16).T
        part_value = nn(probs_low, grad)
        part_key = nn(grad_scores, query)
        if unit == 0:
            dvalue_s[...] = part_value
            dkey_s[...] = part_key
        else:
            dvalue_s[:span, :] += part_value
            dkey_s[:span, :] += part_key
        for head in range(heads_unit):
            lanes = pl.ds((first + head) * dim, dim)
            part = slice(head * block, (head + 1) * block)
            out_ref[step * per:(step + 1) * per, 0, :, lanes] = attn[part].reshape(per, sub, dim)
            back = rope_back(grad_query[part], cos, sin)
            dqkv_ref[step * per:(step + 1) * per, 0, :, lanes] = back.reshape(per, sub, dim)

    count = len(units)
    load(0)
    for unit in range(count + 1):
        if unit < count:
            soften(unit)
        if unit + 1 < count:
            load(unit + 1)
        if unit > 0:
            finish(unit - 1)

    grad_key = (dkey_s[...] * scale).astype(jnp.bfloat16)
    back = rope_back(grad_key, cos_ref[...], sin_ref[...])
    dqkv_ref[:, 0, :, group * dim:(group + 1) * dim] = back.reshape(devs, sub, dim)
    dqkv_ref[:, 0, :, (group + 1) * dim:] = dvalue_s[...].astype(jnp.bfloat16).reshape(devs, sub, dim)


def attention(qkv, grad, cos, sin, heads, name):
    devs, count, sub, width = qkv.shape
    dim = cos.shape[1]
    seq = devs * sub
    per_head = width // heads
    group = per_head // dim - 2

    def head_spec(cols):
        return pl.BlockSpec((devs, 1, sub, cols), lambda b, a: (0, b, 0, a))

    table_spec = pl.BlockSpec((seq, dim), lambda b, a: (0, 0))
    return pl.pallas_call(
        attention_kernel,
        name=name,
        grid=(count, heads),
        in_specs=[head_spec(per_head), head_spec(group * dim), table_spec, table_spec],
        out_specs=[head_spec(group * dim), head_spec(per_head)],
        out_shape=[jax.ShapeDtypeStruct((devs, count, sub, heads * cols), jnp.bfloat16)
                   for cols in (group * dim, per_head)],
        scratch_shapes=[pltpu.VMEM((seq, dim), jnp.float32), pltpu.VMEM((seq, dim), jnp.float32)],
        compiler_params=pltpu.CompilerParams(vmem_limit_bytes=56 * 1024 * 1024),
        cost_estimate=pl.CostEstimate(flops=count * heads * group * 6 * 2 * seq * seq * dim,
                                      bytes_accessed=4 * (qkv.size + grad.size),
                                      transcendentals=count * heads * group * seq * seq // 2),
    )(qkv, grad, cos, sin)


def join_heads(first, mine_ref, other_ref, out_ref, parts, heads):
    width = sum(parts)
    start = 0
    base = 0
    for cols in parts:
        for head in range(heads):
            lanes = slice(head * width + start, head * width + start + cols)
            mine = mine_ref[:, lanes]
            other = other_ref[:, lanes]
            at = base + 2 * head * cols
            out_ref[:, at:at + cols] = jnp.where(first, mine, other)
            out_ref[:, at + cols:at + 2 * cols] = jnp.where(first, other, mine)
        start += cols
        base += 2 * heads * cols


def join_kernel(parts, heads, core_ref, mine_ref, other_ref, out_ref):
    join_heads(core_ref[0] == 0, mine_ref, other_ref, out_ref, parts, heads)


def join_columns(core, mine, other, parts, heads, name):
    rows, half = mine.shape
    tile = 128
    spec = pl.BlockSpec((tile, half), lambda t, core_ref: (t, 0))
    return pl.pallas_call(
        functools.partial(join_kernel, parts, heads),
        name=name,
        grid_spec=pltpu.PrefetchScalarGridSpec(
            num_scalar_prefetch=1, grid=(rows // tile,), in_specs=[spec, spec],
            out_specs=pl.BlockSpec((tile, 2 * half), lambda t, core_ref: (t, 0))),
        out_shape=jax.ShapeDtypeStruct((rows, 2 * half), mine.dtype),
        compiler_params=pltpu.CompilerParams(vmem_limit_bytes=40 * 1024 * 1024),
        cost_estimate=pl.CostEstimate(flops=rows * half * 64, bytes_accessed=4 * rows * half * mine.dtype.itemsize,
                                      transcendentals=0),
    )(core, mine, other)


def project_join_kernel(parts, heads, core_ref, grad_ref, weight_ref, mine_ref, other_ref, out_ref, joined_ref):
    join_heads(core_ref[0] == 0, mine_ref, other_ref, joined_ref, parts, heads)
    out_ref[...] = lax.dot_general(grad_ref[...], weight_ref[...], (((1,), (1,)), ((), ())),
                                   preferred_element_type=jnp.float32).astype(jnp.bfloat16)


def project_and_join(core, grad, weight, mine, other, parts, heads):
    rows, depth = grad.shape
    model = weight.shape[0]
    half = mine.shape[1]
    tile = 256

    def row_spec(cols):
        return pl.BlockSpec((tile, cols), lambda t, core_ref: (t, 0))

    return pl.pallas_call(
        functools.partial(project_join_kernel, parts, heads),
        name='project_and_join',
        grid_spec=pltpu.PrefetchScalarGridSpec(
            num_scalar_prefetch=1, grid=(model // tile,),
            in_specs=[pl.BlockSpec((rows, depth), lambda t, core_ref: (0, 0), pipeline_mode=pl.Buffered(1)),
                      row_spec(depth), row_spec(half), row_spec(half)],
            out_specs=[pl.BlockSpec((rows, tile), lambda t, core_ref: (0, t)), row_spec(2 * half)]),
        out_shape=[jax.ShapeDtypeStruct((rows, model), jnp.bfloat16),
                   jax.ShapeDtypeStruct((model, 2 * half), jnp.float32)],
        compiler_params=pltpu.CompilerParams(vmem_limit_bytes=62 * 1024 * 1024),
        cost_estimate=pl.CostEstimate(flops=2 * rows * depth * model,
                                      bytes_accessed=2 * depth * (rows + model) + 16 * model * half, transcendentals=0),
    )(core, grad, weight, mine, other)


def pick_columns_kernel(core_ref, query_ref, key_ref, value_ref, out_ref):
    query = query_ref.shape[1]
    small = key_ref.shape[1]
    out_ref[:, :query] = query_ref[...]
    out_ref[:, query:query + small] = key_ref[...]
    out_ref[:, query + small:] = value_ref[...]


def pick_columns(core, w_qkv, heads, group, dim):
    rows = w_qkv.shape[0]
    tile = 1024
    width = (group + 2) * dim
    kv_base = 2 * heads * group
    return pl.pallas_call(
        pick_columns_kernel,
        name='pick_columns',
        grid_spec=pltpu.PrefetchScalarGridSpec(
            num_scalar_prefetch=1, grid=(rows // tile, heads),
            in_specs=[pl.BlockSpec((tile, group * dim), lambda t, a, core_ref: (t, 2 * a + core_ref[0])),
                      pl.BlockSpec((tile, dim), lambda t, a, core_ref: (t, kv_base + 2 * a + core_ref[0])),
                      pl.BlockSpec((tile, dim), lambda t, a, core_ref: (t, kv_base + 2 * heads + 2 * a + core_ref[0]))],
            out_specs=pl.BlockSpec((tile, width), lambda t, a, core_ref: (t, a))),
        out_shape=jax.ShapeDtypeStruct((rows, heads * width), w_qkv.dtype),
        compiler_params=pltpu.CompilerParams(vmem_limit_bytes=32 * 1024 * 1024),
        cost_estimate=pl.CostEstimate(flops=rows * heads * width * 32, bytes_accessed=4 * rows * heads * width,
                                      transcendentals=0),
    )(core, w_qkv, w_qkv, w_qkv)


def pick_rows_kernel(core_ref, in_ref, out_ref):
    out_ref[...] = in_ref[...]


def pick_rows(core, w_out, heads, rows):
    cols = w_out.shape[1]
    return pl.pallas_call(
        pick_rows_kernel,
        name='pick_rows',
        grid_spec=pltpu.PrefetchScalarGridSpec(
            num_scalar_prefetch=1, grid=(heads, 2),
            in_specs=[pl.BlockSpec((rows // 2, cols), lambda a, h, core_ref: (4 * a + 2 * core_ref[0] + h, 0))],
            out_specs=pl.BlockSpec((rows // 2, cols), lambda a, h, core_ref: (2 * a + h, 0))),
        out_shape=jax.ShapeDtypeStruct((heads * rows, cols), w_out.dtype),
        compiler_params=pltpu.CompilerParams(vmem_limit_bytes=32 * 1024 * 1024),
        cost_estimate=pl.CostEstimate(flops=heads * rows * cols * 32, bytes_accessed=4 * heads * rows * cols,
                                      transcendentals=0),
    )(core, w_out)


def pick_tokens_kernel(count, devs_ref, *refs):
    inputs, outputs = refs[:2 * count], refs[2 * count:]
    for side in range(2):
        start = 0
        for index in range(count):
            part = inputs[side * count + index]
            outputs[side][start:start + part.shape[1]] = part[0]
            start += part.shape[1]


def pick_tokens(devs, chunks, name):
    sub, width = chunks[0].shape[2:]
    batch = sum(chunk.shape[1] for chunk in chunks)

    def token_spec(chunk, side):
        return pl.BlockSpec((1,) + chunk.shape[1:], lambda g, devs_ref: (devs_ref[side], 0, 0, 0))

    out = jax.ShapeDtypeStruct((batch, sub, width), chunks[0].dtype)
    out_spec = pl.BlockSpec((batch, sub, width), lambda g, devs_ref: (0, 0, 0))
    return pl.pallas_call(
        functools.partial(pick_tokens_kernel, len(chunks)),
        name=name,
        grid_spec=pltpu.PrefetchScalarGridSpec(
            num_scalar_prefetch=1, grid=(1,),
            in_specs=[token_spec(chunk, side) for side in range(2) for chunk in chunks],
            out_specs=[out_spec, out_spec]),
        out_shape=[out, out],
        compiler_params=pltpu.CompilerParams(vmem_limit_bytes=60 * 1024 * 1024),
        cost_estimate=pl.CostEstimate(flops=batch * sub * width * 64, bytes_accessed=8 * batch * sub * width,
                                      transcendentals=0),
    )(devs, *chunks, *chunks)


def exchange_sum(part, devs):
    bit = 1
    while bit < devs:
        part = part + lax.ppermute(part, 'sp', [(d, d ^ bit) for d in range(devs)])
        bit *= 2
    return part


def block_body(hidden, positions, long_factor, norm_weight, w_qkv, w_out, grad_out):
    batch, sub, model = hidden.shape
    dim = 2 * long_factor.shape[0]
    query_dim = w_out.shape[0]
    kv_dim = (w_qkv.shape[1] - query_dim) // 2
    kv_heads = kv_dim // dim
    group = query_dim // kv_dim
    devs = lax.axis_size('sp')
    mine_heads = kv_heads // 2
    me = lax.axis_index('sp')
    core = lax.rem(me, 2)
    chip = lax.div(me, 2)
    partner = me + 1 - 2 * core
    pairs = [(d, d ^ 1) for d in range(devs)]

    hidden_wide = hidden.astype(jnp.float32)
    inv_rms = lax.rsqrt(jnp.mean(hidden_wide * hidden_wide, axis=-1, keepdims=True) + NORM_EPS)
    normed = (hidden_wide * inv_rms * norm_weight).astype(jnp.bfloat16)

    core_ref = core.reshape(1)
    w_own = pick_columns(core_ref, w_qkv, mine_heads, group, dim)
    wo_own = pick_rows(core_ref, w_out, mine_heads, group * dim)
    spread = lax.dynamic_update_slice(jnp.zeros((devs * sub,), positions.dtype), positions, (me * sub,))
    cos, sin = rope_tables(exchange_sum(spread, devs), long_factor)

    gathered = []
    start = 0
    for count in CHUNKS:
        gathered.append((lax.all_gather(normed[start:start + count], 'sp', axis=0),
                         lax.all_gather(grad_out[start:start + count], 'sp', axis=0)))
        start += count

    def project(normed_all):
        return jnp.einsum('tbsd,de->tbse', normed_all, w_own, preferred_element_type=jnp.float32).astype(jnp.bfloat16)

    def project_back(grad_all):
        return jnp.einsum('tbsd,ed->tbse', grad_all, wo_own, preferred_element_type=jnp.float32).astype(jnp.bfloat16)

    def after(value, *earlier):
        *earlier, value = lax.optimization_barrier((*earlier, value))
        return (value, *earlier)

    grad_wqkv = None
    grad_wout = None
    tokens = []
    last = len(CHUNKS) - 1
    for index, (normed_all, grad_all) in enumerate(gathered):
        if index == 0:
            grad_attn = project_back(grad_all)
            normed_all, grad_attn = after(normed_all, grad_attn)
            qkv = project(normed_all)
        else:
            attn, grad_qkv = tokens[-1]
            if index == 1:
                normed_all, attn, grad_wqkv = after(normed_all, attn, grad_wqkv)
            else:
                normed_all, attn = after(normed_all, attn)
            tokens[-1] = (attn, grad_qkv)
            qkv = project(normed_all)
            grad_all, qkv, grad_wout = after(grad_all, qkv, grad_wout)
            grad_attn = project_back(grad_all)
        attn, grad_qkv = attention(qkv, grad_attn, cos, sin, mine_heads, f'attention_{index}')
        tokens.append((attn, grad_qkv))
        attn_slice = lax.dynamic_slice_in_dim(attn, chip * group * dim, group * dim, axis=3)
        part_out = jnp.einsum('tbse,tbsd->ed', attn_slice, grad_all, preferred_element_type=jnp.float32)
        grad_wout = part_out if grad_wout is None else grad_wout + part_out
        if index == last:
            ends = jnp.stack([me, partner])
            picked = [pick_tokens(ends, list(arrays), name) for arrays, name in
                      zip(zip(*tokens), ('pick_attention', 'pick_gradient'))]
            others = [lax.ppermute(pair[1], 'sp', pairs) for pair in picked]
            grad_qkv, *others = after(grad_qkv, *others)
        part_qkv = jnp.einsum('tbsd,tbse->de', normed_all, grad_qkv, preferred_element_type=jnp.float32)
        grad_wqkv = part_qkv if grad_wqkv is None else grad_wqkv + part_qkv

    grad_wqkv_other = lax.ppermute(grad_wqkv, 'sp', pairs)
    grad_wout = lax.all_gather(grad_wout, 'sp', axis=0, tiled=True)
    parts = (group * dim, dim, dim)

    def natural(index, parts, name):
        rows = (batch * sub, -1)
        return join_columns(core_ref, picked[index][0].reshape(rows), others[index].reshape(rows), parts, mine_heads, name)

    attn_flat = natural(0, parts[:1], 'join_attention').reshape(batch, sub, -1)
    mixed_out = jnp.einsum('bse,ed->bsd', attn_flat, w_out, preferred_element_type=jnp.float32)
    out_hidden = (hidden_wide + mixed_out).astype(jnp.bfloat16)

    grad_qkv = natural(1, parts, 'join_gradient')
    grad_qkv, out_hidden = after(grad_qkv, out_hidden)
    grad_normed, grad_wqkv = project_and_join(core_ref, grad_qkv, w_qkv, grad_wqkv, grad_wqkv_other, parts, mine_heads)
    grad_normed = grad_normed.reshape(batch, sub, model).astype(jnp.float32)
    unit_hidden = hidden_wide * inv_rms
    grad_norm = jnp.sum(grad_normed * unit_hidden, axis=(0, 1))
    grad_unit = grad_normed * norm_weight
    grad_inner = inv_rms * (grad_unit - unit_hidden * jnp.mean(grad_unit * unit_hidden, axis=-1, keepdims=True))
    grad_hidden = (grad_out.astype(jnp.float32) + grad_inner).astype(jnp.bfloat16)

    return out_hidden, grad_hidden, exchange_sum(grad_norm, devs), grad_wqkv, grad_wout


def solution(mesh):
    token_spec = P('dp', 'sp', None)
    return jax.shard_map(block_body, mesh=mesh,
                         in_specs=(token_spec, P(('dp', 'sp')), P(), P(), P(), P(), token_spec),
                         out_specs=(token_spec, token_spec, P('dp'), P('dp', None), P('dp', None)),
                         check_vma=False)
```

```python
import functools
import math
import jax
import jax.numpy as jnp
from jax import lax
from jax.experimental import pallas as pl
from jax.experimental.pallas import tpu as pltpu
from jax.sharding import PartitionSpec as P

NORM_EPS = 1e-5
ROPE_BASE = 10000.0
ROPE_SCALE = math.sqrt(1.0 + math.log(32.0) / math.log(4096.0))
LOG2_E = math.log2(math.e)
CHUNKS = (2, 4, 5, 5)
SPLIT_ROWS = 768


def rope_tables(positions, long_factor):
    head_dim = 2 * long_factor.shape[0]
    exponents = jnp.arange(0, head_dim, 2).astype(jnp.float32) / head_dim
    inv_freq = 1.0 / (long_factor * ROPE_BASE ** exponents)
    angles = positions.astype(jnp.float32)[:, None] * inv_freq[None, :]
    cos_half = jnp.cos(angles) * ROPE_SCALE
    sin_half = jnp.sin(angles) * ROPE_SCALE
    return jnp.concatenate([cos_half, cos_half], axis=-1), jnp.concatenate([-sin_half, sin_half], axis=-1)


def attention_kernel(qkv_ref, grad_ref, cos_ref, sin_ref, out_ref, dqkv_ref, dkey_s, dvalue_s):
    devs, _, sub, width = qkv_ref.shape
    dim = cos_ref.shape[1]
    seq = devs * sub
    group = width // dim - 2
    block = 128
    per = block // sub
    scale = dim ** -0.5

    def rope(vals, cos, sin):
        wide = vals.astype(jnp.float32)
        return (wide * cos + pltpu.roll(wide, dim // 2, 1) * sin).astype(jnp.bfloat16)

    def rope_back(vals, cos, sin):
        wide = vals.astype(jnp.float32)
        return (wide * cos - pltpu.roll(wide, dim // 2, 1) * sin).astype(jnp.bfloat16)

    def nt(lhs, rhs):
        return lax.dot_general(lhs, rhs, (((1,), (1,)), ((), ())), preferred_element_type=jnp.float32)

    def nn(lhs, rhs):
        return jnp.dot(lhs, rhs, preferred_element_type=jnp.float32)

    key_raw = qkv_ref[:, 0, :, group * dim:(group + 1) * dim].reshape(seq, dim)
    value = qkv_ref[:, 0, :, (group + 1) * dim:].reshape(seq, dim)
    key = rope(key_raw, cos_ref[...], sin_ref[...])
    key_t = key.T
    value_t = value.T
    heads_unit = 2
    cols = heads_unit * block
    row_ids = lax.broadcasted_iota(jnp.int32, (block, cols), 0)
    col_ids = lax.broadcasted_iota(jnp.int32, (block, cols), 1)
    allowed = row_ids <= lax.rem(col_ids, block)
    units = [(step, first) for step in reversed(range(seq // block)) for first in range(0, group, heads_unit)]
    state = {}

    def load(unit):
        step, first = units[unit]
        rows = pl.ds(step * block, block)
        cos = cos_ref[rows, :]
        sin = sin_ref[rows, :]
        span = (step + 1) * block
        queries = []
        grads = []
        for head in range(first, first + heads_unit):
            lanes = pl.ds(head * dim, dim)
            raw = qkv_ref[step * per:(step + 1) * per, 0, :, lanes].reshape(block, dim)
            queries.append(rope(raw, cos, sin))
            grads.append(grad_ref[step * per:(step + 1) * per, 0, :, lanes].reshape(block, dim))
        query = jnp.concatenate(queries, axis=0)
        grad = jnp.concatenate(grads, axis=0)
        scores = nt(key[:span], query)
        grad_probs = nt(value[:span], grad).astype(jnp.bfloat16)
        state[unit] = (query, grad, scores, grad_probs)

    def soften(unit):
        step, first = units[unit]
        span = (step + 1) * block
        query, grad, scores, grad_probs = state[unit]
        last = jnp.where(allowed, scores[span - block:], -jnp.inf)
        scores = last if step == 0 else jnp.concatenate([scores[:span - block], last], axis=0)
        peak = jnp.max(scores, axis=0, keepdims=True)
        weights = jnp.exp2((scores - peak) * (scale * LOG2_E))
        probs = weights * (1.0 / jnp.sum(weights, axis=0, keepdims=True))
        grad_probs = grad_probs.astype(jnp.float32)
        row_dot = jnp.sum(grad_probs * probs, axis=0, keepdims=True)
        grad_scores = (probs * (grad_probs - row_dot)).astype(jnp.bfloat16)
        state[unit] = (query, grad, probs.astype(jnp.bfloat16), grad_scores)

    def finish(unit):
        step, first = units[unit]
        rows = pl.ds(step * block, block)
        cos = cos_ref[rows, :]
        sin = sin_ref[rows, :]
        span = (step + 1) * block
        query, grad, probs_low, grad_scores = state.pop(unit)
        attn = nn(value_t[:, :span], probs_low).astype(jnp.bfloat16).T
        grad_query = (nn(key_t[:, :span], grad_scores) * scale).astype(jnp.bfloat16).T
        part_value = nn(probs_low, grad)
        part_key = nn(grad_scores, query)
        if unit == 0:
            dvalue_s[...] = part_value
            dkey_s[...] = part_key
        else:
            dvalue_s[:span, :] += part_value
            dkey_s[:span, :] += part_key
        for head in range(heads_unit):
            lanes = pl.ds((first + head) * dim, dim)
            part = slice(head * block, (head + 1) * block)
            out_ref[step * per:(step + 1) * per, 0, :, lanes] = attn[part].reshape(per, sub, dim)
            back = rope_back(grad_query[part], cos, sin)
            dqkv_ref[step * per:(step + 1) * per, 0, :, lanes] = back.reshape(per, sub, dim)

    count = len(units)
    load(0)
    for unit in range(count + 1):
        if unit < count:
            soften(unit)
        if unit + 1 < count:
            load(unit + 1)
        if unit > 0:
            finish(unit - 1)

    grad_key = (dkey_s[...] * scale).astype(jnp.bfloat16)
    back = rope_back(grad_key, cos_ref[...], sin_ref[...])
    dqkv_ref[:, 0, :, group * dim:(group + 1) * dim] = back.reshape(devs, sub, dim)
    dqkv_ref[:, 0, :, (group + 1) * dim:] = dvalue_s[...].astype(jnp.bfloat16).reshape(devs, sub, dim)


def attention(qkv, grad, cos, sin, heads, name):
    devs, count, sub, width = qkv.shape
    dim = cos.shape[1]
    seq = devs * sub
    per_head = width // heads
    group = per_head // dim - 2

    def head_spec(cols):
        return pl.BlockSpec((devs, 1, sub, cols), lambda b, a: (0, b, 0, a))

    table_spec = pl.BlockSpec((seq, dim), lambda b, a: (0, 0))
    return pl.pallas_call(
        attention_kernel,
        name=name,
        grid=(count, heads),
        in_specs=[head_spec(per_head), head_spec(group * dim), table_spec, table_spec],
        out_specs=[head_spec(group * dim), head_spec(per_head)],
        out_shape=[jax.ShapeDtypeStruct((devs, count, sub, heads * cols), jnp.bfloat16)
                   for cols in (group * dim, per_head)],
        scratch_shapes=[pltpu.VMEM((seq, dim), jnp.float32), pltpu.VMEM((seq, dim), jnp.float32)],
        compiler_params=pltpu.CompilerParams(vmem_limit_bytes=56 * 1024 * 1024),
        cost_estimate=pl.CostEstimate(flops=count * heads * group * 6 * 2 * seq * seq * dim,
                                      bytes_accessed=4 * (qkv.size + grad.size),
                                      transcendentals=count * heads * group * seq * seq // 2),
    )(qkv, grad, cos, sin)


def join_heads(first, mine_ref, other_ref, out_ref, parts, heads):
    width = sum(parts)
    start = 0
    base = 0
    for cols in parts:
        for head in range(heads):
            lanes = slice(head * width + start, head * width + start + cols)
            mine = mine_ref[:, lanes]
            other = other_ref[:, lanes]
            at = base + 2 * head * cols
            out_ref[:, at:at + cols] = jnp.where(first, mine, other)
            out_ref[:, at + cols:at + 2 * cols] = jnp.where(first, other, mine)
        start += cols
        base += 2 * heads * cols


def join_kernel(parts, heads, core_ref, mine_ref, other_ref, out_ref):
    join_heads(core_ref[0] == 0, mine_ref, other_ref, out_ref, parts, heads)


def join_columns(core, mine, other, parts, heads, name):
    rows, half = mine.shape
    tile = 128
    spec = pl.BlockSpec((tile, half), lambda t, core_ref: (t, 0))
    return pl.pallas_call(
        functools.partial(join_kernel, parts, heads),
        name=name,
        grid_spec=pltpu.PrefetchScalarGridSpec(
            num_scalar_prefetch=1, grid=(rows // tile,), in_specs=[spec, spec],
            out_specs=pl.BlockSpec((tile, 2 * half), lambda t, core_ref: (t, 0))),
        out_shape=jax.ShapeDtypeStruct((rows, 2 * half), mine.dtype),
        compiler_params=pltpu.CompilerParams(vmem_limit_bytes=40 * 1024 * 1024),
        cost_estimate=pl.CostEstimate(flops=rows * half * 64, bytes_accessed=4 * rows * half * mine.dtype.itemsize,
                                      transcendentals=0),
    )(core, mine, other)


def project_join_kernel(parts, heads, limit, core_ref, grad_ref, weight_ref, mine_ref, other_ref, split_ref,
                        out_ref, joined_ref, sem):
    step = pl.program_id(0)
    core = core_ref[0]
    tile = mine_ref.shape[0]
    rows = pl.ds(pl.multiple_of(step * tile, tile), tile)

    def copies(halves):
        start = 0
        base = 0
        for cols in parts:
            for head in range(2 * heads):
                if halves:
                    half, at = divmod(head, heads)
                    ref = other_ref if half else mine_ref
                    src = ref.at[:, pl.ds(at * sum(parts) + start, cols)]
                    spot = 2 * at + (1 - core if half else core)
                else:
                    src = split_ref.at[head, :, pl.ds(start, cols)]
                    spot = head
                dst = joined_ref.at[rows, pl.ds(pl.multiple_of(base + spot * cols, 128), cols)]
                yield pltpu.make_async_copy(src, dst, sem)
            start += cols
            base += 2 * heads * cols

    @pl.when(step < limit)
    def _():
        for copy in copies(True):
            copy.start()

    @pl.when(step >= limit)
    def _():
        for copy in copies(False):
            copy.start()

    out_ref[...] = lax.dot_general(grad_ref[...], weight_ref[...], (((1,), (1,)), ((), ())),
                                   preferred_element_type=jnp.float32).astype(jnp.bfloat16)

    @pl.when(step < limit)
    def _():
        for copy in copies(True):
            copy.wait()

    @pl.when(step >= limit)
    def _():
        for copy in copies(False):
            copy.wait()


def project_and_join(core, grad, weight, mine, other, split, parts, heads):
    rows, depth = grad.shape
    model = weight.shape[0]
    own, half = mine.shape
    tile = 256
    limit = own // tile

    half_spec = pl.BlockSpec((tile, half), lambda t, core_ref: (jnp.minimum(t, limit - 1), 0))
    return pl.pallas_call(
        functools.partial(project_join_kernel, parts, heads, limit),
        name='project_and_join',
        grid_spec=pltpu.PrefetchScalarGridSpec(
            num_scalar_prefetch=1, grid=(model // tile,),
            in_specs=[pl.BlockSpec((rows, depth), lambda t, core_ref: (0, 0), pipeline_mode=pl.Buffered(1)),
                      pl.BlockSpec((tile, depth), lambda t, core_ref: (t, 0)), half_spec, half_spec,
                      pl.BlockSpec((split.shape[0], tile, split.shape[2]),
                                   lambda t, core_ref: (0, jnp.maximum(t - limit, 0), 0))],
            out_specs=[pl.BlockSpec((rows, tile), lambda t, core_ref: (0, t)), pl.BlockSpec(memory_space=pl.ANY)],
            scratch_shapes=[pltpu.SemaphoreType.DMA]),
        out_shape=[jax.ShapeDtypeStruct((rows, model), jnp.bfloat16),
                   jax.ShapeDtypeStruct((model, 2 * half), jnp.float32)],
        compiler_params=pltpu.CompilerParams(vmem_limit_bytes=62 * 1024 * 1024),
        cost_estimate=pl.CostEstimate(flops=2 * rows * depth * model,
                                      bytes_accessed=2 * depth * (rows + model) + 16 * model * half, transcendentals=0),
    )(core, grad, weight, mine, other, split)


def pick_columns_kernel(core_ref, query_ref, key_ref, value_ref, out_ref):
    query = query_ref.shape[1]
    small = key_ref.shape[1]
    out_ref[:, :query] = query_ref[...]
    out_ref[:, query:query + small] = key_ref[...]
    out_ref[:, query + small:] = value_ref[...]


def pick_columns(core, w_qkv, heads, group, dim):
    rows = w_qkv.shape[0]
    tile = 1024
    width = (group + 2) * dim
    kv_base = 2 * heads * group
    return pl.pallas_call(
        pick_columns_kernel,
        name='pick_columns',
        grid_spec=pltpu.PrefetchScalarGridSpec(
            num_scalar_prefetch=1, grid=(rows // tile, heads),
            in_specs=[pl.BlockSpec((tile, group * dim), lambda t, a, core_ref: (t, 2 * a + core_ref[0])),
                      pl.BlockSpec((tile, dim), lambda t, a, core_ref: (t, kv_base + 2 * a + core_ref[0])),
                      pl.BlockSpec((tile, dim), lambda t, a, core_ref: (t, kv_base + 2 * heads + 2 * a + core_ref[0]))],
            out_specs=pl.BlockSpec((tile, width), lambda t, a, core_ref: (t, a))),
        out_shape=jax.ShapeDtypeStruct((rows, heads * width), w_qkv.dtype),
        compiler_params=pltpu.CompilerParams(vmem_limit_bytes=32 * 1024 * 1024),
        cost_estimate=pl.CostEstimate(flops=rows * heads * width * 32, bytes_accessed=4 * rows * heads * width,
                                      transcendentals=0),
    )(core, w_qkv, w_qkv, w_qkv)


def pick_rows_kernel(core_ref, in_ref, out_ref):
    out_ref[...] = in_ref[...]


def pick_rows(core, w_out, heads, rows):
    cols = w_out.shape[1]
    return pl.pallas_call(
        pick_rows_kernel,
        name='pick_rows',
        grid_spec=pltpu.PrefetchScalarGridSpec(
            num_scalar_prefetch=1, grid=(heads, 2),
            in_specs=[pl.BlockSpec((rows // 2, cols), lambda a, h, core_ref: (4 * a + 2 * core_ref[0] + h, 0))],
            out_specs=pl.BlockSpec((rows // 2, cols), lambda a, h, core_ref: (2 * a + h, 0))),
        out_shape=jax.ShapeDtypeStruct((heads * rows, cols), w_out.dtype),
        compiler_params=pltpu.CompilerParams(vmem_limit_bytes=32 * 1024 * 1024),
        cost_estimate=pl.CostEstimate(flops=heads * rows * cols * 32, bytes_accessed=4 * heads * rows * cols,
                                      transcendentals=0),
    )(core, w_out)


def pick_tokens_kernel(count, devs_ref, *refs):
    inputs, outputs = refs[:2 * count], refs[2 * count:]
    for side in range(2):
        start = 0
        for index in range(count):
            part = inputs[side * count + index]
            outputs[side][start:start + part.shape[1]] = part[0]
            start += part.shape[1]


def pick_tokens(devs, chunks, name):
    sub, width = chunks[0].shape[2:]
    batch = sum(chunk.shape[1] for chunk in chunks)

    def token_spec(chunk, side):
        return pl.BlockSpec((1,) + chunk.shape[1:], lambda g, devs_ref: (devs_ref[side], 0, 0, 0))

    out = jax.ShapeDtypeStruct((batch, sub, width), chunks[0].dtype)
    out_spec = pl.BlockSpec((batch, sub, width), lambda g, devs_ref: (0, 0, 0))
    return pl.pallas_call(
        functools.partial(pick_tokens_kernel, len(chunks)),
        name=name,
        grid_spec=pltpu.PrefetchScalarGridSpec(
            num_scalar_prefetch=1, grid=(1,),
            in_specs=[token_spec(chunk, side) for side in range(2) for chunk in chunks],
            out_specs=[out_spec, out_spec]),
        out_shape=[out, out],
        compiler_params=pltpu.CompilerParams(vmem_limit_bytes=60 * 1024 * 1024),
        cost_estimate=pl.CostEstimate(flops=batch * sub * width * 64, bytes_accessed=8 * batch * sub * width,
                                      transcendentals=0),
    )(devs, *chunks, *chunks)


def exchange_sum(part, devs):
    bit = 1
    while bit < devs:
        part = part + lax.ppermute(part, 'sp', [(d, d ^ bit) for d in range(devs)])
        bit *= 2
    return part


def block_body(hidden, positions, long_factor, norm_weight, w_qkv, w_out, grad_out):
    batch, sub, model = hidden.shape
    dim = 2 * long_factor.shape[0]
    query_dim = w_out.shape[0]
    kv_dim = (w_qkv.shape[1] - query_dim) // 2
    kv_heads = kv_dim // dim
    group = query_dim // kv_dim
    devs = lax.axis_size('sp')
    mine_heads = kv_heads // 2
    me = lax.axis_index('sp')
    core = lax.rem(me, 2)
    chip = lax.div(me, 2)
    partner = me + 1 - 2 * core
    pairs = [(d, d ^ 1) for d in range(devs)]

    hidden_wide = hidden.astype(jnp.float32)
    inv_rms = lax.rsqrt(jnp.mean(hidden_wide * hidden_wide, axis=-1, keepdims=True) + NORM_EPS)
    normed = (hidden_wide * inv_rms * norm_weight).astype(jnp.bfloat16)

    core_ref = core.reshape(1)
    w_own = pick_columns(core_ref, w_qkv, mine_heads, group, dim)
    wo_own = pick_rows(core_ref, w_out, mine_heads, group * dim)
    spread = lax.dynamic_update_slice(jnp.zeros((devs * sub,), positions.dtype), positions, (me * sub,))
    cos, sin = rope_tables(exchange_sum(spread, devs), long_factor)

    gathered = []
    start = 0
    for count in CHUNKS:
        gathered.append((lax.all_gather(normed[start:start + count], 'sp', axis=0),
                         lax.all_gather(grad_out[start:start + count], 'sp', axis=0)))
        start += count

    def project(normed_all):
        return jnp.einsum('tbsd,de->tbse', normed_all, w_own, preferred_element_type=jnp.float32).astype(jnp.bfloat16)

    def project_back(grad_all):
        return jnp.einsum('tbsd,ed->tbse', grad_all, wo_own, preferred_element_type=jnp.float32).astype(jnp.bfloat16)

    def after(value, *earlier):
        *earlier, value = lax.optimization_barrier((*earlier, value))
        return (value, *earlier)

    own_rows = model - SPLIT_ROWS
    width = (group + 2) * dim
    grad_wqkv = None
    grad_split = None
    grad_wout = None
    tokens = []
    last = len(CHUNKS) - 1
    for index, (normed_all, grad_all) in enumerate(gathered):
        if index == 0:
            grad_attn = project_back(grad_all)
            normed_all, grad_attn = after(normed_all, grad_attn)
            qkv = project(normed_all)
        else:
            attn, grad_qkv = tokens[-1]
            if index == 1:
                normed_all, attn, grad_wqkv = after(normed_all, attn, grad_wqkv)
            else:
                normed_all, attn = after(normed_all, attn)
            tokens[-1] = (attn, grad_qkv)
            qkv = project(normed_all)
            grad_all, qkv, grad_wout, grad_split = after(grad_all, qkv, grad_wout, grad_split)
            grad_attn = project_back(grad_all)
        attn, grad_qkv = attention(qkv, grad_attn, cos, sin, mine_heads, f'attention_{index}')
        tokens.append((attn, grad_qkv))
        qkv_slice = lax.dynamic_slice_in_dim(grad_qkv, chip * width, width, axis=3)
        part_split = jnp.einsum('tbsd,tbse->de', normed_all[..., own_rows:], qkv_slice, preferred_element_type=jnp.float32)
        grad_split = part_split if grad_split is None else grad_split + part_split
        attn_slice = lax.dynamic_slice_in_dim(attn, chip * group * dim, group * dim, axis=3)
        if index == last:
            attn_slice, grad_split = after(attn_slice, grad_split)
        part_out = jnp.einsum('tbse,tbsd->ed', attn_slice, grad_all, preferred_element_type=jnp.float32)
        grad_wout = part_out if grad_wout is None else grad_wout + part_out
        if index == last:
            ends = jnp.stack([me, partner])
            picked = [pick_tokens(ends, list(arrays), name) for arrays, name in
                      zip(zip(*tokens), ('pick_attention', 'pick_gradient'))]
            others = [lax.ppermute(pair[1], 'sp', pairs) for pair in picked]
            grad_qkv, *others = after(grad_qkv, *others)
        part_qkv = jnp.einsum('tbsd,tbse->de', normed_all[..., :own_rows], grad_qkv, preferred_element_type=jnp.float32)
        grad_wqkv = part_qkv if grad_wqkv is None else grad_wqkv + part_qkv

    grad_wqkv_other = lax.ppermute(grad_wqkv, 'sp', pairs)
    grad_split = lax.all_gather(grad_split, 'sp', axis=0)
    grad_wout = lax.all_gather(grad_wout, 'sp', axis=0, tiled=True)
    parts = (group * dim, dim, dim)

    def natural(index, parts, name):
        rows = (batch * sub, -1)
        return join_columns(core_ref, picked[index][0].reshape(rows), others[index].reshape(rows), parts, mine_heads, name)

    attn_flat = natural(0, parts[:1], 'join_attention').reshape(batch, sub, -1)
    mixed_out = jnp.einsum('bse,ed->bsd', attn_flat, w_out, preferred_element_type=jnp.float32)
    out_hidden = (hidden_wide + mixed_out).astype(jnp.bfloat16)

    grad_qkv = natural(1, parts, 'join_gradient')
    grad_qkv, out_hidden = after(grad_qkv, out_hidden)
    grad_normed, grad_wqkv = project_and_join(core_ref, grad_qkv, w_qkv, grad_wqkv, grad_wqkv_other, grad_split,
                                              parts, mine_heads)
    grad_normed = grad_normed.reshape(batch, sub, model).astype(jnp.float32)
    unit_hidden = hidden_wide * inv_rms
    grad_norm = jnp.sum(grad_normed * unit_hidden, axis=(0, 1))
    grad_unit = grad_normed * norm_weight
    grad_inner = inv_rms * (grad_unit - unit_hidden * jnp.mean(grad_unit * unit_hidden, axis=-1, keepdims=True))
    grad_hidden = (grad_out.astype(jnp.float32) + grad_inner).astype(jnp.bfloat16)

    return out_hidden, grad_hidden, exchange_sum(grad_norm, devs), grad_wqkv, grad_wout


def solution(mesh):
    token_spec = P('dp', 'sp', None)
    return jax.shard_map(block_body, mesh=mesh,
                         in_specs=(token_spec, P(('dp', 'sp')), P(), P(), P(), P(), token_spec),
                         out_specs=(token_spec, token_spec, P('dp'), P('dp', None), P('dp', None)),
                         check_vma=False)
```

```python
import functools
import math
import jax
import jax.numpy as jnp
from jax import lax
from jax.experimental import pallas as pl
from jax.experimental.pallas import tpu as pltpu
from jax.sharding import PartitionSpec as P

NORM_EPS = 1e-5
ROPE_BASE = 10000.0
ROPE_SCALE = math.sqrt(1.0 + math.log(32.0) / math.log(4096.0))
LOG2_E = math.log2(math.e)
CHUNKS = (2, 4, 5, 5)
SPLIT_ROWS = 768


def rope_tables(positions, long_factor):
    head_dim = 2 * long_factor.shape[0]
    exponents = jnp.arange(0, head_dim, 2).astype(jnp.float32) / head_dim
    inv_freq = 1.0 / (long_factor * ROPE_BASE ** exponents)
    angles = positions.astype(jnp.float32)[:, None] * inv_freq[None, :]
    cos_half = jnp.cos(angles) * ROPE_SCALE
    sin_half = jnp.sin(angles) * ROPE_SCALE
    return jnp.concatenate([cos_half, cos_half], axis=-1), jnp.concatenate([-sin_half, sin_half], axis=-1)


def attention_kernel(group, qkv_ref, grad_ref, cos_ref, sin_ref, out_ref, dqkv_ref, dkey_s, dvalue_s):
    devs, _, sub, width = qkv_ref.shape
    dim = cos_ref.shape[1]
    seq = devs * sub
    per_head = (group + 2) * dim
    block = 128
    per = block // sub
    scale = dim ** -0.5
    heads_unit = 2
    cols = heads_unit * block

    def rope(vals, cos, sin):
        wide = vals.astype(jnp.float32)
        return (wide * cos + pltpu.roll(wide, dim // 2, 1) * sin).astype(jnp.bfloat16)

    def rope_back(vals, cos, sin):
        wide = vals.astype(jnp.float32)
        return (wide * cos - pltpu.roll(wide, dim // 2, 1) * sin).astype(jnp.bfloat16)

    def nt(lhs, rhs):
        return lax.dot_general(lhs, rhs, (((1,), (1,)), ((), ())), preferred_element_type=jnp.float32)

    def nn(lhs, rhs):
        return jnp.dot(lhs, rhs, preferred_element_type=jnp.float32)

    row_ids = lax.broadcasted_iota(jnp.int32, (block, cols), 0)
    col_ids = lax.broadcasted_iota(jnp.int32, (block, cols), 1)
    allowed = row_ids <= lax.rem(col_ids, block)
    units = [(kv, step, first) for kv in range(width // per_head)
             for step in reversed(range(seq // block)) for first in range(0, group, heads_unit)]
    state = {}
    shared = {}

    def load(unit):
        kv, step, first = units[unit]
        base = kv * per_head
        if kv not in shared:
            key_raw = qkv_ref[:, 0, :, base + group * dim:base + (group + 1) * dim].reshape(seq, dim)
            value = qkv_ref[:, 0, :, base + (group + 1) * dim:base + per_head].reshape(seq, dim)
            key = rope(key_raw, cos_ref[...], sin_ref[...])
            shared[kv] = key, value, key.T, value.T
        key, value = shared[kv][:2]
        rows = pl.ds(step * block, block)
        cos = cos_ref[rows, :]
        sin = sin_ref[rows, :]
        span = (step + 1) * block
        queries = []
        grads = []
        for head in range(first, first + heads_unit):
            raw = qkv_ref[step * per:(step + 1) * per, 0, :, pl.ds(base + head * dim, dim)].reshape(block, dim)
            queries.append(rope(raw, cos, sin))
            lanes = pl.ds((kv * group + head) * dim, dim)
            grads.append(grad_ref[step * per:(step + 1) * per, 0, :, lanes].reshape(block, dim))
        query = jnp.concatenate(queries, axis=0)
        grad = jnp.concatenate(grads, axis=0)
        scores = nt(key[:span], query)
        grad_probs = nt(value[:span], grad).astype(jnp.bfloat16)
        state[unit] = (query, grad, scores, grad_probs)

    def soften(unit):
        kv, step, first = units[unit]
        span = (step + 1) * block
        query, grad, scores, grad_probs = state[unit]
        last = jnp.where(allowed, scores[span - block:], -jnp.inf)
        scores = last if step == 0 else jnp.concatenate([scores[:span - block], last], axis=0)
        peak = jnp.max(scores, axis=0, keepdims=True)
        weights = jnp.exp2((scores - peak) * (scale * LOG2_E))
        probs = weights * (1.0 / jnp.sum(weights, axis=0, keepdims=True))
        grad_probs = grad_probs.astype(jnp.float32)
        row_dot = jnp.sum(grad_probs * probs, axis=0, keepdims=True)
        grad_scores = (probs * (grad_probs - row_dot)).astype(jnp.bfloat16)
        state[unit] = (query, grad, probs.astype(jnp.bfloat16), grad_scores)

    def finish(unit):
        kv, step, first = units[unit]
        base = kv * per_head
        key_t, value_t = shared[kv][2:]
        rows = pl.ds(step * block, block)
        cos = cos_ref[rows, :]
        sin = sin_ref[rows, :]
        span = (step + 1) * block
        query, grad, probs_low, grad_scores = state.pop(unit)
        attn = nn(value_t[:, :span], probs_low).astype(jnp.bfloat16).T
        grad_query = (nn(key_t[:, :span], grad_scores) * scale).astype(jnp.bfloat16).T
        part_value = nn(probs_low, grad)
        part_key = nn(grad_scores, query)
        if span == seq and first == 0:
            dvalue_s[kv] = part_value
            dkey_s[kv] = part_key
        else:
            dvalue_s[kv, :span, :] += part_value
            dkey_s[kv, :span, :] += part_key
        for head in range(heads_unit):
            part = slice(head * block, (head + 1) * block)
            lanes = pl.ds((kv * group + first + head) * dim, dim)
            out_ref[step * per:(step + 1) * per, 0, :, lanes] = attn[part].reshape(per, sub, dim)
            back = rope_back(grad_query[part], cos, sin)
            lanes = pl.ds(base + (first + head) * dim, dim)
            dqkv_ref[step * per:(step + 1) * per, 0, :, lanes] = back.reshape(per, sub, dim)
        if step == 0 and first + heads_unit == group:
            grad_key = (dkey_s[kv] * scale).astype(jnp.bfloat16)
            back = rope_back(grad_key, cos_ref[...], sin_ref[...])
            dqkv_ref[:, 0, :, base + group * dim:base + (group + 1) * dim] = back.reshape(devs, sub, dim)
            last = dvalue_s[kv].astype(jnp.bfloat16).reshape(devs, sub, dim)
            dqkv_ref[:, 0, :, base + (group + 1) * dim:base + per_head] = last

    count = len(units)
    load(0)
    for unit in range(count + 1):
        if unit < count:
            soften(unit)
        if unit + 1 < count:
            load(unit + 1)
        if unit > 0:
            finish(unit - 1)


def attention(qkv, grad, cos, sin, heads, name, kvs=2):
    devs, count, sub, width = qkv.shape
    dim = cos.shape[1]
    seq = devs * sub
    per_head = width // heads
    group = per_head // dim - 2

    def head_spec(cols):
        return pl.BlockSpec((devs, 1, sub, kvs * cols), lambda b, a: (0, b, 0, a))

    table_spec = pl.BlockSpec((seq, dim), lambda b, a: (0, 0))
    return pl.pallas_call(
        functools.partial(attention_kernel, group),
        name=name,
        grid=(count, heads // kvs),
        in_specs=[head_spec(per_head), head_spec(group * dim), table_spec, table_spec],
        out_specs=[head_spec(group * dim), head_spec(per_head)],
        out_shape=[jax.ShapeDtypeStruct((devs, count, sub, heads * cols), jnp.bfloat16)
                   for cols in (group * dim, per_head)],
        scratch_shapes=[pltpu.VMEM((kvs, seq, dim), jnp.float32), pltpu.VMEM((kvs, seq, dim), jnp.float32)],
        compiler_params=pltpu.CompilerParams(vmem_limit_bytes=56 * 1024 * 1024),
        cost_estimate=pl.CostEstimate(flops=count * heads * group * 6 * 2 * seq * seq * dim,
                                      bytes_accessed=4 * (qkv.size + grad.size),
                                      transcendentals=count * heads * group * seq * seq // 2),
    )(qkv, grad, cos, sin)


def join_heads(first, mine_ref, other_ref, out_ref, parts, heads):
    width = sum(parts)
    start = 0
    base = 0
    for cols in parts:
        for head in range(heads):
            lanes = slice(head * width + start, head * width + start + cols)
            mine = mine_ref[:, lanes]
            other = other_ref[:, lanes]
            at = base + 2 * head * cols
            out_ref[:, at:at + cols] = jnp.where(first, mine, other)
            out_ref[:, at + cols:at + 2 * cols] = jnp.where(first, other, mine)
        start += cols
        base += 2 * heads * cols


def join_kernel(parts, heads, core_ref, mine_ref, other_ref, out_ref):
    join_heads(core_ref[0] == 0, mine_ref, other_ref, out_ref, parts, heads)


def join_columns(core, mine, other, parts, heads, name):
    rows, half = mine.shape
    tile = 128
    spec = pl.BlockSpec((tile, half), lambda t, core_ref: (t, 0))
    return pl.pallas_call(
        functools.partial(join_kernel, parts, heads),
        name=name,
        grid_spec=pltpu.PrefetchScalarGridSpec(
            num_scalar_prefetch=1, grid=(rows // tile,), in_specs=[spec, spec],
            out_specs=pl.BlockSpec((tile, 2 * half), lambda t, core_ref: (t, 0))),
        out_shape=jax.ShapeDtypeStruct((rows, 2 * half), mine.dtype),
        compiler_params=pltpu.CompilerParams(vmem_limit_bytes=40 * 1024 * 1024),
        cost_estimate=pl.CostEstimate(flops=rows * half * 64, bytes_accessed=4 * rows * half * mine.dtype.itemsize,
                                      transcendentals=0),
    )(core, mine, other)


def project_join_kernel(parts, heads, limit, core_ref, grad_ref, weight_ref, mine_ref, other_ref, split_ref,
                        out_ref, joined_ref, sem):
    step = pl.program_id(0)
    core = core_ref[0]
    tile = mine_ref.shape[0]
    rows = pl.ds(pl.multiple_of(step * tile, tile), tile)

    def copies(halves):
        start = 0
        base = 0
        for cols in parts:
            for head in range(2 * heads):
                if halves:
                    half, at = divmod(head, heads)
                    ref = other_ref if half else mine_ref
                    src = ref.at[:, pl.ds(at * sum(parts) + start, cols)]
                    spot = 2 * at + (1 - core if half else core)
                else:
                    src = split_ref.at[head, :, pl.ds(start, cols)]
                    spot = head
                dst = joined_ref.at[rows, pl.ds(pl.multiple_of(base + spot * cols, 128), cols)]
                yield pltpu.make_async_copy(src, dst, sem)
            start += cols
            base += 2 * heads * cols

    @pl.when(step < limit)
    def _():
        for copy in copies(True):
            copy.start()

    @pl.when(step >= limit)
    def _():
        for copy in copies(False):
            copy.start()

    out_ref[...] = lax.dot_general(grad_ref[...], weight_ref[...], (((1,), (1,)), ((), ())),
                                   preferred_element_type=jnp.float32).astype(jnp.bfloat16)

    @pl.when(step < limit)
    def _():
        for copy in copies(True):
            copy.wait()

    @pl.when(step >= limit)
    def _():
        for copy in copies(False):
            copy.wait()


def project_and_join(core, grad, weight, mine, other, split, parts, heads):
    rows, depth = grad.shape
    model = weight.shape[0]
    own, half = mine.shape
    tile = 256
    limit = own // tile

    half_spec = pl.BlockSpec((tile, half), lambda t, core_ref: (jnp.minimum(t, limit - 1), 0))
    return pl.pallas_call(
        functools.partial(project_join_kernel, parts, heads, limit),
        name='project_and_join',
        grid_spec=pltpu.PrefetchScalarGridSpec(
            num_scalar_prefetch=1, grid=(model // tile,),
            in_specs=[pl.BlockSpec((rows, depth), lambda t, core_ref: (0, 0), pipeline_mode=pl.Buffered(1)),
                      pl.BlockSpec((tile, depth), lambda t, core_ref: (t, 0)), half_spec, half_spec,
                      pl.BlockSpec((split.shape[0], tile, split.shape[2]),
                                   lambda t, core_ref: (0, jnp.maximum(t - limit, 0), 0))],
            out_specs=[pl.BlockSpec((rows, tile), lambda t, core_ref: (0, t)), pl.BlockSpec(memory_space=pl.ANY)],
            scratch_shapes=[pltpu.SemaphoreType.DMA]),
        out_shape=[jax.ShapeDtypeStruct((rows, model), jnp.bfloat16),
                   jax.ShapeDtypeStruct((model, 2 * half), jnp.float32)],
        compiler_params=pltpu.CompilerParams(vmem_limit_bytes=62 * 1024 * 1024),
        cost_estimate=pl.CostEstimate(flops=2 * rows * depth * model,
                                      bytes_accessed=2 * depth * (rows + model) + 16 * model * half, transcendentals=0),
    )(core, grad, weight, mine, other, split)


def output_kernel(attn_ref, weight_ref, hidden_ref, half_ref, out_ref, full_ref, sem):
    tile, cols = half_ref.shape
    rows = pl.ds(pl.multiple_of(pl.program_id(0) * tile, tile), tile)
    copy = pltpu.make_async_copy(half_ref, full_ref.at[rows, pl.ds(0, cols)], sem)
    copy.start()
    mixed = jnp.dot(attn_ref[...], weight_ref[...], preferred_element_type=jnp.float32)
    out_ref[...] = (hidden_ref[...].astype(jnp.float32) + mixed).astype(jnp.bfloat16)
    copy.wait()


def output_and_copy(attn, weight, hidden, half):
    rows, depth = attn.shape
    model = weight.shape[1]
    total, cols = half.shape
    steps = 8
    tile = model // steps
    return pl.pallas_call(
        output_kernel,
        name='output_and_copy',
        grid=(steps,),
        in_specs=[pl.BlockSpec((rows, depth), lambda t: (0, 0), pipeline_mode=pl.Buffered(1)),
                  pl.BlockSpec((depth, tile), lambda t: (0, t)), pl.BlockSpec((rows, tile), lambda t: (0, t)),
                  pl.BlockSpec((total // steps, cols), lambda t: (t, 0))],
        out_specs=[pl.BlockSpec((rows, tile), lambda t: (0, t)), pl.BlockSpec(memory_space=pl.ANY)],
        out_shape=[jax.ShapeDtypeStruct((rows, model), jnp.bfloat16),
                   jax.ShapeDtypeStruct((total, 2 * cols), jnp.float32)],
        scratch_shapes=[pltpu.SemaphoreType.DMA],
        compiler_params=pltpu.CompilerParams(vmem_limit_bytes=60 * 1024 * 1024),
        cost_estimate=pl.CostEstimate(flops=2 * rows * depth * model,
                                      bytes_accessed=2 * depth * (rows + model) + 8 * total * cols, transcendentals=0),
    )(attn, weight, hidden, half)


def second_half_kernel(left_ref, half_ref, full_ref, sem):
    tile, cols = half_ref.shape
    rows = pl.ds(pl.multiple_of(pl.program_id(0) * tile, tile), tile)
    copy = pltpu.make_async_copy(half_ref, full_ref.at[rows, pl.ds(cols, cols)], sem)
    copy.start()
    copy.wait()


def second_half(full, half):
    total, cols = half.shape
    steps = 8
    return pl.pallas_call(
        second_half_kernel,
        name='second_half',
        grid=(steps,),
        in_specs=[pl.BlockSpec(memory_space=pl.ANY), pl.BlockSpec((total // steps, cols), lambda t: (t, 0))],
        out_specs=pl.BlockSpec(memory_space=pl.ANY),
        out_shape=jax.ShapeDtypeStruct(full.shape, full.dtype),
        scratch_shapes=[pltpu.SemaphoreType.DMA],
        input_output_aliases={0: 0},
        compiler_params=pltpu.CompilerParams(vmem_limit_bytes=32 * 1024 * 1024),
        cost_estimate=pl.CostEstimate(flops=32 * total * cols, bytes_accessed=8 * total * cols, transcendentals=0),
    )(full, half)


def pick_columns_kernel(core_ref, query_ref, key_ref, value_ref, out_ref):
    query = query_ref.shape[1]
    small = key_ref.shape[1]
    out_ref[:, :query] = query_ref[...]
    out_ref[:, query:query + small] = key_ref[...]
    out_ref[:, query + small:] = value_ref[...]


def pick_columns(core, w_qkv, heads, group, dim):
    rows = w_qkv.shape[0]
    tile = 1024
    width = (group + 2) * dim
    kv_base = 2 * heads * group
    return pl.pallas_call(
        pick_columns_kernel,
        name='pick_columns',
        grid_spec=pltpu.PrefetchScalarGridSpec(
            num_scalar_prefetch=1, grid=(rows // tile, heads),
            in_specs=[pl.BlockSpec((tile, group * dim), lambda t, a, core_ref: (t, 2 * a + core_ref[0])),
                      pl.BlockSpec((tile, dim), lambda t, a, core_ref: (t, kv_base + 2 * a + core_ref[0])),
                      pl.BlockSpec((tile, dim), lambda t, a, core_ref: (t, kv_base + 2 * heads + 2 * a + core_ref[0]))],
            out_specs=pl.BlockSpec((tile, width), lambda t, a, core_ref: (t, a))),
        out_shape=jax.ShapeDtypeStruct((rows, heads * width), w_qkv.dtype),
        compiler_params=pltpu.CompilerParams(vmem_limit_bytes=32 * 1024 * 1024),
        cost_estimate=pl.CostEstimate(flops=rows * heads * width * 32, bytes_accessed=4 * rows * heads * width,
                                      transcendentals=0),
    )(core, w_qkv, w_qkv, w_qkv)


def pick_rows_kernel(core_ref, in_ref, out_ref):
    out_ref[...] = in_ref[...]


def pick_rows(core, w_out, heads, rows):
    cols = w_out.shape[1]
    return pl.pallas_call(
        pick_rows_kernel,
        name='pick_rows',
        grid_spec=pltpu.PrefetchScalarGridSpec(
            num_scalar_prefetch=1, grid=(heads, 2),
            in_specs=[pl.BlockSpec((rows // 2, cols), lambda a, h, core_ref: (4 * a + 2 * core_ref[0] + h, 0))],
            out_specs=pl.BlockSpec((rows // 2, cols), lambda a, h, core_ref: (2 * a + h, 0))),
        out_shape=jax.ShapeDtypeStruct((heads * rows, cols), w_out.dtype),
        compiler_params=pltpu.CompilerParams(vmem_limit_bytes=32 * 1024 * 1024),
        cost_estimate=pl.CostEstimate(flops=heads * rows * cols * 32, bytes_accessed=4 * heads * rows * cols,
                                      transcendentals=0),
    )(core, w_out)


def pick_tokens_kernel(count, devs_ref, *refs):
    inputs, outputs = refs[:2 * count], refs[2 * count:]
    for side in range(2):
        start = 0
        for index in range(count):
            part = inputs[side * count + index]
            outputs[side][start:start + part.shape[1]] = part[0]
            start += part.shape[1]


def pick_tokens(devs, chunks, name):
    sub, width = chunks[0].shape[2:]
    batch = sum(chunk.shape[1] for chunk in chunks)

    def token_spec(chunk, side):
        return pl.BlockSpec((1,) + chunk.shape[1:], lambda g, devs_ref: (devs_ref[side], 0, 0, 0))

    out = jax.ShapeDtypeStruct((batch, sub, width), chunks[0].dtype)
    out_spec = pl.BlockSpec((batch, sub, width), lambda g, devs_ref: (0, 0, 0))
    return pl.pallas_call(
        functools.partial(pick_tokens_kernel, len(chunks)),
        name=name,
        grid_spec=pltpu.PrefetchScalarGridSpec(
            num_scalar_prefetch=1, grid=(1,),
            in_specs=[token_spec(chunk, side) for side in range(2) for chunk in chunks],
            out_specs=[out_spec, out_spec]),
        out_shape=[out, out],
        compiler_params=pltpu.CompilerParams(vmem_limit_bytes=60 * 1024 * 1024),
        cost_estimate=pl.CostEstimate(flops=batch * sub * width * 64, bytes_accessed=8 * batch * sub * width,
                                      transcendentals=0),
    )(devs, *chunks, *chunks)


def exchange_sum(part, devs):
    bit = 1
    while bit < devs:
        part = part + lax.ppermute(part, 'sp', [(d, d ^ bit) for d in range(devs)])
        bit *= 2
    return part


def block_body(hidden, positions, long_factor, norm_weight, w_qkv, w_out, grad_out):
    batch, sub, model = hidden.shape
    dim = 2 * long_factor.shape[0]
    query_dim = w_out.shape[0]
    kv_dim = (w_qkv.shape[1] - query_dim) // 2
    kv_heads = kv_dim // dim
    group = query_dim // kv_dim
    devs = lax.axis_size('sp')
    mine_heads = kv_heads // 2
    me = lax.axis_index('sp')
    core = lax.rem(me, 2)
    chip = lax.div(me, 2)
    partner = me + 1 - 2 * core
    pairs = [(d, d ^ 1) for d in range(devs)]

    hidden_wide = hidden.astype(jnp.float32)
    inv_rms = lax.rsqrt(jnp.mean(hidden_wide * hidden_wide, axis=-1, keepdims=True) + NORM_EPS)
    normed = (hidden_wide * inv_rms * norm_weight).astype(jnp.bfloat16)

    core_ref = core.reshape(1)
    w_own = pick_columns(core_ref, w_qkv, mine_heads, group, dim)
    wo_own = pick_rows(core_ref, w_out, mine_heads, group * dim)
    spread = lax.dynamic_update_slice(jnp.zeros((devs * sub,), positions.dtype), positions, (me * sub,))
    cos, sin = rope_tables(exchange_sum(spread, devs), long_factor)

    gathered = []
    start = 0
    for count in CHUNKS:
        gathered.append((lax.all_gather(normed[start:start + count], 'sp', axis=0),
                         lax.all_gather(grad_out[start:start + count], 'sp', axis=0)))
        start += count

    def project(normed_all):
        return jnp.einsum('tbsd,de->tbse', normed_all, w_own, preferred_element_type=jnp.float32).astype(jnp.bfloat16)

    def project_back(grad_all):
        return jnp.einsum('tbsd,ed->tbse', grad_all, wo_own, preferred_element_type=jnp.float32).astype(jnp.bfloat16)

    def after(value, *earlier):
        *earlier, value = lax.optimization_barrier((*earlier, value))
        return (value, *earlier)

    own_rows = model - SPLIT_ROWS
    width = (group + 2) * dim
    grad_wqkv = None
    grad_split = None
    grad_wout = [None, None]
    tokens = []
    last = len(CHUNKS) - 1
    for index, (normed_all, grad_all) in enumerate(gathered):
        if index == 0:
            grad_attn = project_back(grad_all)
            normed_all, grad_attn = after(normed_all, grad_attn)
            qkv = project(normed_all)
        else:
            attn, grad_qkv = tokens[-1]
            if index == 1:
                normed_all, attn, grad_wqkv = after(normed_all, attn, grad_wqkv)
            else:
                normed_all, attn = after(normed_all, attn)
            tokens[-1] = (attn, grad_qkv)
            qkv = project(normed_all)
            grad_all, qkv, *grad_wout, grad_split = after(grad_all, qkv, *grad_wout, grad_split)
            grad_attn = project_back(grad_all)
        attn, grad_qkv = attention(qkv, grad_attn, cos, sin, mine_heads, f'attention_{index}')
        tokens.append((attn, grad_qkv))
        qkv_slice = lax.dynamic_slice_in_dim(grad_qkv, chip * width, width, axis=3)
        part_split = jnp.einsum('tbsd,tbse->de', normed_all[..., own_rows:], qkv_slice, preferred_element_type=jnp.float32)
        grad_split = part_split if grad_split is None else grad_split + part_split
        attn_slice = lax.dynamic_slice_in_dim(attn, chip * group * dim, group * dim, axis=3)
        if index == last:
            attn_slice, grad_split = after(attn_slice, grad_split)
        for side in range(2):
            lanes = slice(side * model // 2, (side + 1) * model // 2)
            part_out = jnp.einsum('tbse,tbsd->ed', attn_slice, grad_all[..., lanes], preferred_element_type=jnp.float32)
            grad_wout[side] = part_out if grad_wout[side] is None else grad_wout[side] + part_out
        if index == last:
            ends = jnp.stack([me, partner])
            picked = [pick_tokens(ends, list(arrays), name) for arrays, name in
                      zip(zip(*tokens), ('pick_attention', 'pick_gradient'))]
            others = [lax.ppermute(pair[1], 'sp', pairs) for pair in picked]
            grad_qkv, *others = after(grad_qkv, *others)
        part_qkv = jnp.einsum('tbsd,tbse->de', normed_all[..., :own_rows], grad_qkv, preferred_element_type=jnp.float32)
        grad_wqkv = part_qkv if grad_wqkv is None else grad_wqkv + part_qkv

    grad_wqkv_other = lax.ppermute(grad_wqkv, 'sp', pairs)
    grad_split = lax.all_gather(grad_split, 'sp', axis=0)
    grad_wout = [lax.all_gather(half, 'sp', axis=0, tiled=True) for half in grad_wout]
    parts = (group * dim, dim, dim)

    def natural(index, parts, name):
        rows = (batch * sub, -1)
        return join_columns(core_ref, picked[index][0].reshape(rows), others[index].reshape(rows), parts, mine_heads, name)

    attn_flat = natural(0, parts[:1], 'join_attention')
    out_hidden, grad_wout_full = output_and_copy(attn_flat, w_out, hidden.reshape(batch * sub, model), grad_wout[0])
    out_hidden = out_hidden.reshape(batch, sub, model)

    grad_qkv = natural(1, parts, 'join_gradient')
    grad_qkv, out_hidden = after(grad_qkv, out_hidden)
    grad_normed, grad_wqkv = project_and_join(core_ref, grad_qkv, w_qkv, grad_wqkv, grad_wqkv_other, grad_split,
                                              parts, mine_heads)
    grad_normed = grad_normed.reshape(batch, sub, model).astype(jnp.float32)
    unit_hidden = hidden_wide * inv_rms
    grad_norm = jnp.sum(grad_normed * unit_hidden, axis=(0, 1))
    grad_unit = grad_normed * norm_weight
    grad_inner = inv_rms * (grad_unit - unit_hidden * jnp.mean(grad_unit * unit_hidden, axis=-1, keepdims=True))
    grad_hidden = (grad_out.astype(jnp.float32) + grad_inner).astype(jnp.bfloat16)

    grad_wout = second_half(grad_wout_full, grad_wout[1])
    return out_hidden, grad_hidden, exchange_sum(grad_norm, devs), grad_wqkv, grad_wout


def solution(mesh):
    token_spec = P('dp', 'sp', None)
    return jax.shard_map(block_body, mesh=mesh,
                         in_specs=(token_spec, P(('dp', 'sp')), P(), P(), P(), P(), token_spec),
                         out_specs=(token_spec, token_spec, P('dp'), P('dp', None), P('dp', None)),
                         check_vma=False)
```
